256 devices in a mesh: seq: 32 (over y, z), tp: 8 (over x, core).
Axes of the slice: x: 4, y: 4, z: 8, core: 2. Of those that a mesh axis runs over, the one named last changes fastest.
Arguments:
- tokens: bfloat16 [16384, 2560], P('seq', 'tp'), may hold values from -6 to 6
- gate_weight: bfloat16 [2560, 5120], P(None, 'tp'), may hold values from -0.125 to 0.125
- inner_weight: bfloat16 [2560, 5120], P(None, 'tp'), may hold values from -0.125 to 0.125
- state_weight: bfloat16 [2560, 256], replicated, may hold values from -0.125 to 0.125
- step_weight: bfloat16 [2560, 80], P(None, 'tp'), may hold values from -0.125 to 0.125
- conv_inner: float32 [4, 5120], P(None, 'tp'), may hold values from -3 to 3
- conv_state: float32 [4, 256], replicated, may hold values from -3 to 3
- step_bias: float32 [80], P('tp'), may hold values from -3 to 1
- decay_rate: float32 [80], P('tp'), may hold values from 1e-05 to 0.02
- skip_gain: float32 [80], P('tp'), may hold values from 0.5 to 2
- norm_gain: float32 [5120], P('tp'), may hold values from 0.1 to 1.9
- out_weight: bfloat16 [5120, 2560], P('tp'), may hold values from -0.078125 to 0.078125
Outputs:
- layer_out: bfloat16 [16384, 2560], P(('seq', 'tp'))
The draws below stay inside these ranges and needn't reach their ends.
All inputs are finite; a program needn't handle non-finite values.
Results may differ from the reference program's by a relative error of at most 0.018.
Values may be sent and summed in bfloat16 or wider, within the bound.
A program may use at most 128 MiB of HBM per device.

```python
import math
import jax
import jax.numpy as jnp
from jax import lax

D = 2560
HEADS = 80
HEAD_DIM = 64
STATE = 128
KERNEL = 4
GROUP = 256
INNER = 5120
TOKENS = 16384


def block_levels(stream_key, shape, shards, smallest, top_value):
    def one(position, parts):
        steps = jax.random.uniform(jax.random.fold_in(jax.random.fold_in(stream_key, 6), position), (parts,), jnp.float32, smallest / len(shards), top_value / len(shards))
        return jnp.repeat(jnp.exp(steps), shape[position] // parts).reshape((-1,) + (1,) * (len(shape) - position - 1))

    level = one(*shards[0])
    for cut in shards[1:]:
        level = level * one(*cut)
    return level


def centred(rng, shape, width, reach, split=(), kind=jnp.bfloat16):
    array = width * jax.random.normal(rng, shape, jnp.float32)
    if split:
        array = array * block_levels(rng, shape, split, -0.22, 0.18)
    return jnp.clip(array, -reach, reach).astype(kind)


def setup_inputs(seed: int = 0) -> dict:
    key_list = jax.random.split(jax.random.key(seed), 13)
    return {
        "tokens": centred(key_list[0], (TOKENS, D), 1.0, 6.0, ((0, 32), (1, 8))),
        "gate_weight": centred(key_list[1], (D, INNER), D ** -0.5, 0.125, ((1, 8),)),
        "inner_weight": centred(key_list[2], (D, INNER), D ** -0.5, 0.125, ((1, 8),)),
        "state_weight": centred(key_list[3], (D, 2 * STATE), D ** -0.5, 0.125),
        "step_weight": centred(key_list[4], (D, HEADS), D ** -0.5, 0.125, ((1, 8),)),
        "conv_inner": centred(key_list[5], (KERNEL, INNER), KERNEL ** -0.5, 3.0, ((1, 8),), jnp.float32),
        "conv_state": centred(key_list[6], (KERNEL, 2 * STATE), KERNEL ** -0.5, 3.0, (), jnp.float32),
        "step_bias": jnp.clip(-3.0 + 4.0 * jax.random.uniform(key_list[7], (HEADS,), jnp.float32) ** block_levels(key_list[7], (HEADS,), ((0, 8),), -0.2, 0.2), -3.0, 1.0),
        "decay_rate": jnp.clip(jnp.exp(math.log(0.02) - 7.6009025 * jax.random.uniform(key_list[8], (HEADS,), jnp.float32) ** block_levels(key_list[8], (HEADS,), ((0, 8),), -0.2, 0.2)), 9.999999747378752e-06, 0.02),
        "skip_gain": jnp.clip(0.5 + 1.5 * jax.random.uniform(key_list[9], (HEADS,), jnp.float32) ** block_levels(key_list[9], (HEADS,), ((0, 8),), -0.2, 0.2), 0.5, 2.0),
        "norm_gain": jnp.clip(1.0 + 0.18 * jax.random.normal(key_list[10], (INNER,), jnp.float32), 0.1, 1.9),
        "out_weight": centred(key_list[11], (INNER, D), INNER ** -0.5, 0.078125, ((0, 8),)),
    }


def reference(tokens, gate_weight, inner_weight, state_weight, step_weight, conv_inner, conv_state, step_bias, decay_rate, skip_gain, norm_gain, out_weight):
    gate_act = jnp.dot(tokens, gate_weight, preferred_element_type=jnp.float32).astype(jnp.bfloat16)
    mixed_in = jnp.concatenate([jnp.dot(tokens, inner_weight, preferred_element_type=jnp.float32), jnp.dot(tokens, state_weight, preferred_element_type=jnp.float32)], axis=1).astype(jnp.bfloat16)
    step_raw = jnp.dot(tokens, step_weight, preferred_element_type=jnp.float32)
    kernel = jnp.concatenate([conv_inner, conv_state], axis=1)
    padded = jnp.concatenate([jnp.zeros((KERNEL - 1, mixed_in.shape[1]), jnp.bfloat16), mixed_in], axis=0)
    conv_sum = jnp.zeros(mixed_in.shape, jnp.float32)
    for tap in range(KERNEL):
        conv_sum = conv_sum + padded[tap:tap + TOKENS].astype(jnp.float32) * kernel[tap][None, :]
    conv_out = jax.nn.silu(conv_sum).astype(jnp.bfloat16)
    inner_act = conv_out[:, :INNER].reshape(TOKENS, HEADS, HEAD_DIM)
    inject = conv_out[:, INNER:INNER + STATE]
    readout = conv_out[:, INNER + STATE:]
    time_step = jax.nn.softplus(step_raw + step_bias[None, :])
    log_decay = -time_step * decay_rate[None, :]
    blocks = TOKENS // GROUP
    causal = jnp.arange(GROUP)[:, None] >= jnp.arange(GROUP)[None, :]
    highest = lax.Precision.HIGHEST

    def advance(carried, block):
        inner_blk, inject_blk, readout_blk, step_blk, log_blk = block
        cumulative = jnp.cumsum(log_blk, axis=0)
        scores = jnp.dot(readout_blk, inject_blk.T, preferred_element_type=jnp.float32)
        log_gaps = cumulative.T[:, :, None] - cumulative.T[:, None, :]
        decay_mask = jnp.exp(jnp.where(causal[None], log_gaps, -jnp.inf))
        mixing = (scores[None] * decay_mask * step_blk.T[:, None, :]).astype(jnp.bfloat16)
        intra_out = jnp.einsum('hts,shp->thp', mixing.astype(jnp.float32), inner_blk.astype(jnp.float32), precision=highest)
        state_reads = jnp.einsum('tn,hpn->thp', readout_blk.astype(jnp.float32), carried, precision=highest) * jnp.exp(cumulative)[:, :, None]
        ending = cumulative[-1]
        tail_weight = jnp.exp(ending[None, :] - cumulative) * step_blk
        contribution = jnp.einsum('thp,tn->hpn', inner_blk.astype(jnp.float32) * tail_weight[:, :, None], inject_blk.astype(jnp.float32), precision=highest)
        carried = jnp.exp(ending)[:, None, None] * carried + contribution
        return (carried, intra_out + state_reads)
    start_state = jnp.zeros((HEADS, HEAD_DIM, STATE), jnp.float32)
    stacked = (inner_act.reshape(blocks, GROUP, HEADS, HEAD_DIM), inject.reshape(blocks, GROUP, STATE), readout.reshape(blocks, GROUP, STATE), time_step.reshape(blocks, GROUP, HEADS), log_decay.reshape(blocks, GROUP, HEADS))
    final_state, block_outs = lax.scan(advance, start_state, stacked)
    ssd_out = block_outs.reshape(TOKENS, HEADS, HEAD_DIM) + skip_gain[None, :, None] * inner_act.astype(jnp.float32)
    gated = ssd_out.reshape(TOKENS, INNER) * jax.nn.silu(gate_act.astype(jnp.float32))
    mean_square = lax.optimization_barrier(jnp.mean(gated * gated, axis=1))
    normed = (gated * lax.rsqrt(mean_square + 1e-05)[:, None] * norm_gain[None, :]).astype(jnp.bfloat16)
    return jnp.dot(normed, out_weight, preferred_element_type=jnp.float32).astype(jnp.bfloat16)
```

```python
import jax
import jax.numpy as jnp
from jax import lax
from jax.experimental import pallas as pl
from jax.experimental.pallas import tpu as pltpu
from jax.sharding import PartitionSpec as P

MESH = pl.DeviceIdType.MESH
F32 = jnp.float32
BF16 = jnp.bfloat16
ROWS = 512
GROUP = 256
KD = 320
D = 2560
CH = 640
HD = 10
ST = 128
CONV = CH + 2 * ST
QC = 640
NQ = D // QC
LOG2E = 1.4426950408889634
INNER = 5120


def split2(v):
    hi = v.astype(BF16)
    return hi, (v - hi.astype(F32)).astype(BF16)


def dot(a, b):
    return jnp.dot(a, b, preferred_element_type=F32)


def dot_nt(a, b):
    return lax.dot_general(a, b, (((1,), (1,)), ((), ())), preferred_element_type=F32)


def silu(v):
    return 0.5 * v * (1.0 + jnp.tanh(0.5 * v))


def kernel(
    tok, w_gate, w_inner, w_state, w_step, k_inner, k_state, bias, rate, skip, gain, w_out,
    out,
    xb, wg, wi, ws, wt, wo,
    acc_i, acc_s, acc_t, acc_g, mx, act, edge_s, edge_r,
    small, expand, cum_s, dt_s, cumt_s, dtt_s,
    ssd, gexp, st_bf, st_f, c0_s, z_recv, t_send, t_recv, pref, y_send, yt_send, y_recv, yt_recv, f_send, inc, carr,
    gated, sq_send, sq_recv, keep, d_send, d_recv, r1_send, r1_recv, r2_send, fin_l, fin_r, scale_s,
    loc_sem, g_send, g_recv, e_sem, zs_sem, zr_sem, ts_sem, tr_sem, ys_sem, yr_sem, yts_sem, ytr_sem, fs_sem, fr_sem,
    qs_sem, qr_sem, ds_sem, dr_sem, rs_sem, rr_sem,
):
    seq = lax.axis_index("seq")
    tp = lax.axis_index("tp")
    x = tp // 2
    c = tp % 2
    y = seq // 8
    z = seq % 8
    partner = 2 * x + (1 - c)
    rx, lx, ox = (x + 1) % 4, (x + 3) % 4, (x + 2) % 4
    right, left, opp = 2 * rx + c, 2 * lx + c, 2 * ox + c
    nxt, prv = (seq + 1) % 32, (seq + 31) % 32

    def remote(src, dst, ssem, rsem, **where):
        return pltpu.make_async_remote_copy(
            src_ref=src, dst_ref=dst, send_sem=ssem, recv_sem=rsem, device_id=where, device_id_type=MESH
        )

    loads = [
        pltpu.make_async_copy(tok, xb.at[tp], loc_sem.at[0]),
        pltpu.make_async_copy(w_inner, wi, loc_sem.at[1]),
        pltpu.make_async_copy(w_state, ws, loc_sem.at[2]),
        pltpu.make_async_copy(w_step, wt, loc_sem.at[3]),
        pltpu.make_async_copy(w_gate, wg, loc_sem.at[4]),
        pltpu.make_async_copy(w_out, wo, loc_sem.at[5]),
    ]
    for load in loads:
        load.start()

    barrier = pltpu.get_barrier_semaphore()
    for k in range(1, 8):
        pl.semaphore_signal(barrier, inc=1, device_id={"tp": (tp + k) % 8}, device_id_type=MESH)
    for k in range(1, 8):
        pl.semaphore_signal(barrier, inc=1, device_id={"seq": y * 8 + (z + k) % 8}, device_id_type=MESH)
    for k in range(1, 4):
        pl.semaphore_signal(barrier, inc=1, device_id={"seq": ((y + k) % 4) * 8 + z}, device_id_type=MESH)
    for s in (nxt, prv):
        pl.semaphore_signal(barrier, inc=1, device_id={"seq": s}, device_id_type=MESH)

    er = lax.broadcasted_iota(jnp.int32, (ST, CH), 0)
    ec = lax.broadcasted_iota(jnp.int32, (ST, CH), 1)
    off = ec - er * 64
    expand[...] = jnp.where((off >= 0) & (off < 64), 1.0, 0.0).astype(BF16)
    small[...] = jnp.zeros_like(small)
    small[0:1, 0:HD] = bias[...]
    small[8:9, 0:HD] = rate[...]
    small[16:17, 0:HD] = skip[...]
    acc_t[...] = jnp.zeros_like(acc_t)

    def expanded(v):
        hi, lo = split2(v)
        return dot(hi, expand[...]) + dot(lo, expand[...])

    loads[0].wait()
    pl.semaphore_wait(barrier, 19)

    def piece(src, half, to, ssem):
        part = xb.at[src, pl.ds(half * GROUP, GROUP), :]
        return remote(part, part, ssem, g_recv.at[src, half], tp=to)

    sent = []

    def send(src, half, to, ssem):
        copy = piece(src, half, to, ssem)
        copy.start()
        sent.append(copy)

    def arrived(src, half):
        piece(src, half, partner, g_send.at[0]).wait_recv()

    send(tp, 0, right, g_send.at[0])
    send(tp, 1, left, g_send.at[1])
    send(tp, 1, right, g_send.at[2])
    send(tp, 0, left, g_send.at[3])
    send(tp, 0, partner, g_send.at[4])
    send(tp, 1, partner, g_send.at[5])
    for load in loads[1:4]:
        load.wait()

    def accumulate(src, first):
        rows = pl.ds(pl.multiple_of(src * KD, 64), KD)
        for half in range(2):
            rr = pl.ds(half * GROUP, GROUP)
            xs = xb[src, rr, :]
            for n in range(0, CH, 128 * 5):
                v = dot(xs, wi[rows, :])
                acc_i[rr, :] = v if first else acc_i[rr, :] + v
            v = dot(xs, ws[rows, :])
            acc_s[rr, :] = v if first else acc_s[rr, :] + v
            v = dot(xs, wt[rows, :])
            acc_t[rr, 0:HD] = v if first else acc_t[rr, 0:HD] + v

    accumulate(tp, True)
    arrived(left, 0)
    send(left, 0, right, g_send.at[6])
    send(left, 0, partner, g_send.at[7])
    arrived(right, 1)
    send(right, 1, left, g_send.at[8])
    send(right, 1, partner, g_send.at[9])
    arrived(partner, 0)
    arrived(partner, 1)
    accumulate(partner, False)
    arrived(left, 1)
    send(left, 1, partner, g_send.at[10])
    arrived(right, 0)
    send(right, 0, partner, g_send.at[11])

    def loop_accumulate(chips, which):
        def body(i, carry):
            accumulate(2 * jnp.where(i == 0, chips[0], chips[-1]) + which, False)
            return carry

        lax.fori_loop(0, len(chips), body, 0)

    loop_accumulate((lx, rx), c)
    for half in range(2):
        arrived(2 * lx + 1 - c, half)
        arrived(2 * rx + 1 - c, half)
    loop_accumulate((lx, rx), 1 - c)
    arrived(opp, 0)
    send(opp, 0, partner, g_send.at[12])
    arrived(opp, 1)
    send(opp, 1, partner, g_send.at[13])
    accumulate(opp, False)
    arrived(2 * ox + 1 - c, 0)
    arrived(2 * ox + 1 - c, 1)
    accumulate(2 * ox + 1 - c, False)

    edge_s[:, 0:CH] = acc_i[ROWS - 16 : ROWS, :].astype(BF16)
    edge_s[:, CH:CONV] = acc_s[ROWS - 16 : ROWS, :].astype(BF16)
    edge = remote(edge_s, edge_r, e_sem.at[0], e_sem.at[1], seq=nxt)
    edge.start()
    mx[8 : 8 + ROWS, 0:CH] = acc_i[...].astype(BF16).astype(F32)
    mx[8 : 8 + ROWS, CH:CONV] = acc_s[...].astype(BF16).astype(F32)

    tri = (
        lax.broadcasted_iota(jnp.int32, (GROUP, GROUP), 0) >= lax.broadcasted_iota(jnp.int32, (GROUP, GROUP), 1)
    ).astype(F32)
    for b in range(2):
        rr = slice(b * GROUP, (b + 1) * GROUP)
        raw = acc_t[rr, :] + small[0:1, :]
        dt = jnp.maximum(raw, 0.0) + jnp.log1p(jnp.exp(-jnp.abs(raw)))
        ld = -dt * small[8:9, :]
        cum = lax.dot_general(
            tri, ld, (((1,), (0,)), ((), ())), precision=lax.Precision.HIGHEST, preferred_element_type=F32
        )
        cum_s[rr, :] = cum
        dt_s[rr, :] = dt
        cumt_s[b] = (cum * LOG2E).T[0:16, :]
        dtt_s[b] = dt.T[0:16, :]
        gexp[rr, :] = expanded(jnp.exp(cum))

    def conv(b):
        def body(j, carry):
            cols = pl.ds(pl.multiple_of(j * 128, 128), 128)

            def taps(ref, kcols):
                total = mx[pl.ds(b * GROUP + 5, GROUP), cols] * ref[0:1, kcols]
                for k in range(1, 4):
                    total = total + mx[pl.ds(b * GROUP + 5 + k, GROUP), cols] * ref[k : k + 1, kcols]
                return silu(total).astype(BF16)

            act[pl.ds(b * GROUP, GROUP), cols] = taps(kern, cols)
            return carry

        lax.fori_loop(0, CONV // 128, body, 0)

    kern = pref
    kern[0:4, 0:CH] = k_inner[...]
    kern[0:4, CH:CONV] = k_state[...]

    def contribution(b):
        rr = slice(b * GROUP, (b + 1) * GROUP)
        ending = cum_s[(b + 1) * GROUP - 1 : (b + 1) * GROUP, :]
        tail = jnp.exp(ending - cum_s[rr, :]) * dt_s[rr, :]
        scaled = (act[rr, 0:CH].astype(F32) * expanded(tail)).astype(BF16)
        inject_t = act[rr, CH : CH + ST].astype(F32).T.astype(BF16)
        return dot(inject_t, scaled)

    conv(1)
    c1 = contribution(1)
    st_f[...] = c1
    edge.wait_recv()
    halo = edge_r[8:16, :].astype(F32)
    mx[0:8, :] = jnp.where(seq == 0, 0.0, halo)
    conv(0)
    c0_s[...] = contribution(0)
    ends = jnp.concatenate([cum_s[GROUP - 1 : GROUP, :], cum_s[ROWS - 1 : ROWS, :]], axis=0)
    ends8 = jnp.concatenate([ends, jnp.zeros((6, ST), F32)], axis=0)
    end_exp = expanded(jnp.exp(ends8))
    st_bf[...] = (end_exp[1:2, :] * c0_s[...] + st_f[...]).astype(BF16)
    total = ends[0:1, :] + ends[1:2, :]
    row8 = lax.broadcasted_iota(jnp.int32, (8, ST), 0)
    t_send[...] = jnp.where(row8 == z, total, 0.0)

    def zcopy(k):
        to = (z + k) % 8
        return (
            remote(st_bf.at[pl.ds(pl.multiple_of(16 * to, 16), 16), :], z_recv.at[z], zs_sem.at[k], zr_sem.at[z],
                   seq=y * 8 + to),
            remote(t_send, t_recv.at[z], ts_sem.at[k], tr_sem.at[z], seq=y * 8 + to),
        )

    for k in range(1, 8):
        for copy in zcopy(k):
            copy.start()
            sent.append(copy)
    z_recv[z] = st_bf[pl.ds(pl.multiple_of(16 * z, 16), 16), :]
    t_recv[z] = t_send[...]

    def intra(b, rr0):
        t0 = pl.ds(rr0, 128)
        t1 = pl.ds(rr0 + 128, 128)
        both = pl.ds(rr0, GROUP)
        inject = act[both, CH : CH + ST]
        sc0 = dot_nt(act[t0, CH + ST : CONV], inject[0:128, :])
        sc1 = dot_nt(act[t1, CH + ST : CONV], inject)
        diag = lax.broadcasted_iota(jnp.int32, (128, 128), 0) >= lax.broadcasted_iota(jnp.int32, (128, 128), 1)
        lane = lax.broadcasted_iota(jnp.int32, (128, 128), 1) < 64
        ca = cum_s[t0, :] * LOG2E
        cb = cum_s[t1, :] * LOG2E
        for p in range(HD // 2):
            cols = slice(p * 128, (p + 1) * 128)
            chan = act[both, cols]
            res0, res1 = [], []
            for h in (2 * p, 2 * p + 1):
                ct = cumt_s[b, h : h + 1, :]
                dtr = dtt_s[b, h : h + 1, :]
                g0 = jnp.where(diag, ca[:, h : h + 1] - ct[:, 0:128], -1e30)
                m0 = (sc0 * jnp.exp2(g0) * dtr[:, 0:128]).astype(BF16)
                res0.append(dot(m0, chan[0:128, :]))
                g1 = cb[:, h : h + 1] - ct[:, 0:128]
                m1 = (sc1[:, 0:128] * jnp.exp2(g1) * dtr[:, 0:128]).astype(BF16)
                g2 = jnp.where(diag, cb[:, h : h + 1] - ct[:, 128:256], -1e30)
                m2 = (sc1[:, 128:256] * jnp.exp2(g2) * dtr[:, 128:256]).astype(BF16)
                res1.append(dot(m1, chan[0:128, :]) + dot(m2, chan[128:256, :]))
            ssd[t0, cols] = jnp.where(lane, res0[0], res0[1])
            ssd[t1, cols] = jnp.where(lane, res1[0], res1[1])

    def intra_body(b, carry):
        intra(b, pl.multiple_of(b * GROUP, GROUP))
        return carry

    lax.fori_loop(0, 2, intra_body, 0)

    for k in range(1, 8):
        src = (z + k) % 8
        remote(st_bf.at[0:16, :], z_recv.at[src], zs_sem.at[k], zr_sem.at[src], seq=prv).wait_recv()
        remote(t_send, t_recv.at[src], ts_sem.at[k], tr_sem.at[src], seq=prv).wait_recv()
    tall = t_recv[0]
    for k in range(1, 8):
        tall = tall + t_recv[k]
    texp = expanded(jnp.exp(tall))
    prefix = jnp.zeros((16, CH), F32)
    tsum = jnp.zeros((1, ST), F32)
    tpre = []
    for k in range(8):
        f_pre = prefix
        pref[16 * k : 16 * (k + 1), 0:CH] = f_pre
        tpre.append(tsum)
        prefix = texp[k : k + 1, :] * prefix + z_recv[k].astype(F32)
        tsum = tsum + tall[k : k + 1, :]
    y_send[...] = prefix.astype(BF16)
    yt_send[...] = jnp.where(row8 == y, tsum, 0.0)
    for k in range(1, 4):
        to = ((y + k) % 4) * 8 + z
        a = remote(y_send, y_recv.at[y], ys_sem.at[k], yr_sem.at[y], seq=to)
        b = remote(yt_send, yt_recv.at[y], yts_sem.at[k], ytr_sem.at[y], seq=to)
        for copy in (a, b):
            copy.start()
            sent.append(copy)
    y_recv[y] = y_send[...]
    yt_recv[y] = yt_send[...]

    loads[4].wait()

    def gate_body(half, carry):
        rr = pl.ds(pl.multiple_of(half * GROUP, GROUP), GROUP)
        v = dot(xb[0, rr, :], wg[0:KD, :])
        for src in range(1, 8):
            v = v + dot(xb[src, rr, :], wg[src * KD : (src + 1) * KD, :])
        acc_g[rr, :] = silu(v.astype(BF16).astype(F32))
        return carry

    lax.fori_loop(0, 2, gate_body, 0)

    for k in range(1, 4):
        src = (y + k) % 4
        remote(y_send, y_recv.at[src], ys_sem.at[k], yr_sem.at[src], seq=prv).wait_recv()
        remote(yt_send, yt_recv.at[src], yts_sem.at[k], ytr_sem.at[src], seq=prv).wait_recv()
    yall = yt_recv[0]
    for k in range(1, 4):
        yall = yall + yt_recv[k]
    yexp = expanded(jnp.exp(yall))
    run = jnp.zeros((16, CH), F32)
    chosen = run
    for k in range(3):
        run = yexp[k : k + 1, :] * run + y_recv[k].astype(F32)
        chosen = jnp.where(y == k + 1, run, chosen)
    pexp = expanded(jnp.exp(jnp.concatenate(tpre, axis=0)))
    for k in range(8):
        f_send[k] = (pref[16 * k : 16 * (k + 1), 0:CH] + pexp[k : k + 1, :] * chosen).astype(BF16)
    mine = pl.ds(pl.multiple_of(16 * z, 16), 16)
    for k in range(1, 8):
        to = (z + k) % 8
        copy = remote(f_send.at[to], inc.at[mine, :], fs_sem.at[k], fr_sem.at[z], seq=y * 8 + to)
        copy.start()
        sent.append(copy)
    inc[mine, :] = f_send[z]

    skips = expanded(small[16:24, :])[0:1, :]
    ssd[...] = ssd[...] + skips * act[:, 0:CH].astype(F32)
    loads[5].wait()

    for k in range(1, 8):
        src = (z + k) % 8
        there = pl.ds(pl.multiple_of(16 * src, 16), 16)
        remote(f_send.at[0], inc.at[there, :], fs_sem.at[k], fr_sem.at[src], seq=prv).wait_recv()
    carr[0] = inc[...]
    carr[1] = (c0_s[...] + end_exp[0:1, :] * inc[...].astype(F32)).astype(BF16)

    ones = jnp.ones((8, CH), BF16)

    def gated_body(i, carry):
        rr = pl.ds(pl.multiple_of(i * 128, 128), 128)
        reads = dot(act[rr, CH + ST : CONV], carr[i // 2])
        g = (ssd[rr, :] + reads * gexp[rr, :]) * acc_g[rr, :]
        hi, lo = split2(g * g)
        sq_send[i] = dot_nt(ones, hi) + dot_nt(ones, lo)
        gb = (g * gain[...]).astype(BF16)
        to = pl.ds(pl.multiple_of(i * 64, 64), 64)
        gated[0, to, :] = gb[0:64, :]
        gated[1, to, :] = gb[64:128, :]
        return carry

    lax.fori_loop(0, 4, gated_body, 0)
    for k in range(1, 8):
        to = (tp + k) % 8
        copy = remote(sq_send.at[to // 2], sq_recv.at[tp], qs_sem.at[k], qr_sem.at[tp], tp=to)
        copy.start()
        sent.append(copy)
    sq_recv[tp] = sq_send[x]

    def dcopy(q):
        return remote(d_send.at[q], d_recv.at[q], ds_sem.at[q], dr_sem.at[q], tp=partner)

    def block(chip):
        return pl.ds(pl.multiple_of(64 * chip, 64), 64)

    def started(copy):
        copy.start()
        sent.append(copy)

    for q in range(NQ):
        wcols = wo[:, q * QC : (q + 1) * QC]
        d_send[q] = dot(gated[1 - c], wcols).astype(BF16)
        started(dcopy(q))
        keep[q] = dot(gated[c], wcols)

    def hop1(q):
        to = right if q % 2 == 0 else left
        return remote(r1_send.at[q, 0], r1_recv.at[q], rs_sem.at[q, 0], rr_sem.at[q, 0], tp=to)

    def direct(q):
        if q % 2 == 0:
            return remote(r1_send.at[q, 1], fin_r.at[q], rs_sem.at[q, 1], rr_sem.at[q, 1], tp=left)
        return remote(r1_send.at[q, 1], fin_l.at[q], rs_sem.at[q, 1], rr_sem.at[q, 1], tp=right)

    def hop2(q):
        if q % 2 == 0:
            return remote(r2_send.at[q], fin_l.at[q], rs_sem.at[q, 2], rr_sem.at[q, 2], tp=right)
        return remote(r2_send.at[q], fin_r.at[q], rs_sem.at[q, 2], rr_sem.at[q, 2], tp=left)

    for q in range(NQ):
        dcopy(q).wait_recv()
        keep[q] = keep[q] + d_recv[q].astype(F32)
        r1_send[q, 0] = keep[q, block(ox), :].astype(BF16)
        started(hop1(q))
        other = lx if q % 2 == 0 else rx
        r1_send[q, 1] = keep[q, block(other), :].astype(BF16)
        started(direct(q))
    for q in range(NQ):
        hop1(q).wait_recv()
        ahead = rx if q % 2 == 0 else lx
        r2_send[q] = (keep[q, block(ahead), :] + r1_recv[q].astype(F32)).astype(BF16)
        started(hop2(q))

    for k in range(1, 8):
        src = (tp + k) % 8
        remote(sq_send.at[0], sq_recv.at[src], qs_sem.at[k], qr_sem.at[src], tp=partner).wait_recv()
    sq = sq_recv[0]
    for k in range(1, 8):
        sq = sq + sq_recv[k]
    factor = lax.rsqrt(sq * (1.0 / INNER) + 1e-5)
    scale_s[...] = jnp.broadcast_to(factor[0:1, :], (128, 128)).T
    scale = scale_s[block(c), :]
    for q in range(NQ):
        direct(q).wait_recv()
        hop2(q).wait_recv()
        v = keep[q, block(x), :] + fin_l[q].astype(F32) + fin_r[q].astype(F32)
        for j in range(QC // 128):
            cols = slice(j * 128, (j + 1) * 128)
            out[:, q * QC + j * 128 : q * QC + (j + 1) * 128] = (v[:, cols] * scale).astype(BF16)
    edge.wait_send()
    for copy in sent:
        copy.wait_send()


def on_device(tok, w_gate, w_inner, w_state, w_step, k_inner, k_state, bias, rate, skip, gain, w_out):
    vm = pltpu.VMEM
    dma = pltpu.SemaphoreType.DMA
    scratch = [
        vm((8, ROWS, KD), BF16), vm((D, CH), BF16), vm((D, CH), BF16), vm((D, 2 * ST), BF16), vm((D, HD), BF16),
        vm((CH, D), BF16),
        vm((ROWS, CH), F32), vm((ROWS, 2 * ST), F32), vm((ROWS, ST), F32), vm((ROWS, CH), F32),
        vm((8 + ROWS, CONV), F32), vm((ROWS, CONV), BF16), vm((16, CONV), BF16), vm((16, CONV), BF16),
        vm((24, ST), F32), vm((ST, CH), BF16), vm((ROWS, ST), F32), vm((ROWS, ST), F32),
        vm((2, 16, GROUP), F32), vm((2, 16, GROUP), F32),
        vm((ROWS, CH), F32), vm((ROWS, CH), F32), vm((ST, CH), BF16), vm((ST, CH), F32), vm((ST, CH), F32),
        vm((8, 16, CH), BF16), vm((8, ST), F32), vm((8, 8, ST), F32), vm((ST, CONV), F32),
        vm((16, CH), BF16), vm((8, ST), F32), vm((4, 16, CH), BF16), vm((4, 8, ST), F32),
        vm((8, 16, CH), BF16), vm((ST, CH), BF16), vm((2, ST, CH), BF16),
        vm((2, GROUP, CH), BF16), vm((4, 8, ST), F32), vm((8, 8, ST), F32),
        vm((NQ, GROUP, QC), F32), vm((NQ, GROUP, QC), BF16), vm((NQ, GROUP, QC), BF16),
        vm((NQ, 2, 64, QC), BF16), vm((NQ, 64, QC), BF16), vm((NQ, 64, QC), BF16),
        vm((NQ, 64, QC), BF16), vm((NQ, 64, QC), BF16), vm((128, 128), F32),
        dma((6,)), dma((14,)), dma((8, 2)), dma((2,)), dma((8,)), dma((8,)), dma((8,)), dma((8,)),
        dma((4,)), dma((4,)), dma((4,)), dma((4,)), dma((8,)), dma((8,)),
        dma((8,)), dma((8,)), dma((NQ,)), dma((NQ,)), dma((NQ, 3)), dma((NQ, 3)),
    ]
    hbm = pl.BlockSpec(memory_space=pl.ANY)
    local = pl.BlockSpec(memory_space=pltpu.VMEM)
    return pl.pallas_call(
        kernel,
        name="layer",
        out_shape=jax.ShapeDtypeStruct((ROWS // 8, D), BF16),
        in_specs=[hbm] * 5 + [local] * 6 + [hbm],
        out_specs=local,
        scratch_shapes=scratch,
        compiler_params=pltpu.CompilerParams(
            collective_id=0, has_side_effects=True, vmem_limit_bytes=62 * 1024 * 1024
        ),
    )(
        tok, w_gate, w_inner, w_state, w_step, k_inner, k_state,
        bias.reshape(1, -1), rate.reshape(1, -1), skip.reshape(1, -1), gain.reshape(1, -1), w_out,
    )


def solution(mesh):
    return jax.shard_map(
        on_device,
        mesh=mesh,
        in_specs=(
            P("seq", "tp"), P(None, "tp"), P(None, "tp"), P(), P(None, "tp"), P(None, "tp"), P(),
            P("tp"), P("tp"), P("tp"), P("tp"), P("tp", None),
        ),
        out_specs=P(("seq", "tp"), None),
        check_vma=False,
    )
```

```python
import jax
import jax.numpy as jnp
from jax import lax
from jax.experimental import pallas as pl
from jax.experimental.pallas import tpu as pltpu
from jax.sharding import PartitionSpec as P

MESH = pl.DeviceIdType.MESH
F32 = jnp.float32
BF16 = jnp.bfloat16
ROWS = 512
GROUP = 256
KD = 320
D = 2560
CH = 640
HD = 10
ST = 128
CONV = CH + 2 * ST
WIDE = CONV + ST
CUTS = ((0, 512), (1280, 512), (512, 768), (1792, 768))
NQ = len(CUTS)
QC = 768
LOG2E = 1.4426950408889634
INNER = 5120


def split2(v):
    hi = v.astype(BF16)
    return hi, (v - hi.astype(F32)).astype(BF16)


def dot(a, b):
    return jnp.dot(a, b, preferred_element_type=F32)


def dot_nt(a, b):
    return lax.dot_general(a, b, (((1,), (1,)), ((), ())), preferred_element_type=F32)


class Phases:
    open_scope = None

    def __call__(self, name):
        self.close()
        self.open_scope = jax.named_scope(name)
        self.open_scope.__enter__()

    def close(self):
        if self.open_scope is not None:
            self.open_scope.__exit__(None, None, None)
            self.open_scope = None


def silu(v):
    return 0.5 * v * (1.0 + jnp.tanh(0.5 * v))


def kernel(
    tok, w_gate, w_inner, w_state, w_step, k_inner, k_state, bias, rate, skip, gain, w_out,
    out,
    xb, tok_t, step_t, step_f, wg, wall, wo, kern, vec, gain_v,
    acc, acc_g, mx, act, edge_s, edge_r,
    small, expand, cum_s, dt_s, cumt_s, dtt_s,
    ssd, gexp, st_bf, st_f, c0_s, z_recv, t_send, t_recv, pref, y_send, yt_send, y_recv, yt_recv, f_send, inc, carr,
    sq_send, sq_recv, both, keep, d_send, d_recv, r1_send, r1_recv, fin_l, fin_r, scale_s,
    loc_sem, g_send, g_recv, e_sem, zs_sem, zr_sem, ts_sem, tr_sem, ys_sem, yr_sem, yts_sem, ytr_sem, fs_sem, fr_sem,
    qs_sem, qr_sem, ds_sem, dr_sem, rs_sem, rr_sem,
):
    seq = lax.axis_index("seq")
    tp = lax.axis_index("tp")
    x = tp // 2
    c = tp % 2
    y = seq // 8
    z = seq % 8
    partner = 2 * x + (1 - c)
    rx, lx, ox = (x + 1) % 4, (x + 3) % 4, (x + 2) % 4
    right, left, opp = 2 * rx + c, 2 * lx + c, 2 * ox + c
    nxt, prv = (seq + 1) % 32, (seq + 31) % 32

    def remote(src, dst, ssem, rsem, **where):
        return pltpu.make_async_remote_copy(
            src_ref=src, dst_ref=dst, send_sem=ssem, recv_sem=rsem, device_id=where, device_id_type=MESH
        )

    phase = Phases()
    phase("start")
    copies = (
        (tok, tok_t), (w_inner, wall.at[:, 0:CH]), (w_state, wall.at[:, CH:CONV]), (w_step, step_t),
        (k_inner, kern.at[:, 0:CH]), (k_state, kern.at[:, CH:CONV]), (bias, vec.at[0:1]), (rate, vec.at[1:2]),
        (skip, vec.at[2:3]), (gain, gain_v), (w_gate, wg), (w_out, wo),
    )
    loads = [pltpu.make_async_copy(src, dst, loc_sem.at[i]) for i, (src, dst) in enumerate(copies)]
    for load in loads:
        load.start()

    barrier = pltpu.get_barrier_semaphore()
    for k in range(1, 8):
        pl.semaphore_signal(barrier, inc=1, device_id={"tp": (tp + k) % 8}, device_id_type=MESH)
    for k in range(1, 8):
        pl.semaphore_signal(barrier, inc=1, device_id={"seq": y * 8 + (z + k) % 8}, device_id_type=MESH)
    for k in range(1, 4):
        pl.semaphore_signal(barrier, inc=1, device_id={"seq": ((y + k) % 4) * 8 + z}, device_id_type=MESH)
    for s in (nxt, prv):
        pl.semaphore_signal(barrier, inc=1, device_id={"seq": s}, device_id_type=MESH)

    er = lax.broadcasted_iota(jnp.int32, (ST, CH), 0)
    ec = lax.broadcasted_iota(jnp.int32, (ST, CH), 1)
    off = ec - er * 64
    expand[...] = jnp.where((off >= 0) & (off < 64), 1.0, 0.0).astype(BF16)
    small[...] = jnp.zeros_like(small)

    def expanded(v):
        hi, lo = split2(v)
        return dot(hi, expand[...]) + dot(lo, expand[...])

    phase("turn")
    loads[0].wait()
    xb[tp] = tok_t[...].T
    phase("barrier")
    pl.semaphore_wait(barrier, 19)

    phase("send")
    def piece(src, half, to, ssem):
        part = xb.at[src, pl.ds(half * GROUP, GROUP), :]
        return remote(part, part, ssem, g_recv.at[src, half], tp=to)

    sent = []

    def send(src, half, to, ssem):
        copy = piece(src, half, to, ssem)
        copy.start()
        sent.append(copy)

    def arrived(src, half):
        piece(src, half, partner, g_send.at[0]).wait_recv()

    send(tp, 0, right, g_send.at[0])
    send(tp, 1, left, g_send.at[1])
    send(tp, 1, right, g_send.at[2])
    send(tp, 0, left, g_send.at[3])
    send(tp, 0, partner, g_send.at[4])
    send(tp, 1, partner, g_send.at[5])
    phase("step_turn")
    loads[3].wait()
    step_f[...] = jnp.zeros_like(step_f)
    step_f[0:HD, :] = step_t[...].astype(F32)
    wall[:, CONV:WIDE] = step_f[...].T.astype(BF16)
    for i in (6, 7, 8):
        loads[i].wait()
        small[8 * (i - 6) : 8 * (i - 6) + 1, 0:HD] = vec[i - 6 : i - 5, :]
    loads[1].wait()
    loads[2].wait()

    def accumulate(src, half, first=False):
        rr = pl.ds(half * GROUP, GROUP)
        v = dot(xb[src, rr, :], wall[pl.ds(pl.multiple_of(src * KD, 64), KD), :])
        acc[rr, :] = v if first else acc[rr, :] + v

    rp, lp, op = 2 * rx + 1 - c, 2 * lx + 1 - c, 2 * ox + 1 - c
    phase("own")
    accumulate(tp, 0, True)
    accumulate(tp, 1, True)
    for half in range(2):
        arrived(partner, half)
        accumulate(partner, half)
    phase("near0")
    arrived(left, 0)
    send(left, 0, right, g_send.at[6])
    send(left, 0, partner, g_send.at[7])
    arrived(right, 1)
    send(right, 1, left, g_send.at[8])
    send(right, 1, partner, g_send.at[9])
    phase("near0_acc")
    accumulate(left, 0)
    accumulate(right, 1)
    arrived(lp, 0)
    accumulate(lp, 0)
    arrived(rp, 1)
    accumulate(rp, 1)
    phase("near1")
    arrived(left, 1)
    send(left, 1, partner, g_send.at[10])
    arrived(right, 0)
    send(right, 0, partner, g_send.at[11])
    phase("near1_acc")
    accumulate(left, 1)
    accumulate(right, 0)
    arrived(lp, 1)
    accumulate(lp, 1)
    arrived(rp, 0)
    accumulate(rp, 0)
    phase("far")
    arrived(opp, 0)
    send(opp, 0, partner, g_send.at[12])
    arrived(opp, 1)
    send(opp, 1, partner, g_send.at[13])
    phase("far_acc")
    accumulate(opp, 0)
    accumulate(opp, 1)
    phase("far_p")
    for half in range(2):
        arrived(op, half)
        accumulate(op, half)

    phase("edge")
    edge_s[...] = acc[ROWS - 16 : ROWS, 0:CONV].astype(BF16)
    edge = remote(edge_s, edge_r, e_sem.at[0], e_sem.at[1], seq=nxt)
    edge.start()
    mx[8 : 8 + ROWS, :] = acc[:, 0:CONV].astype(BF16).astype(F32)

    phase("steps")
    tri = (
        lax.broadcasted_iota(jnp.int32, (GROUP, GROUP), 0) >= lax.broadcasted_iota(jnp.int32, (GROUP, GROUP), 1)
    ).astype(F32)
    for b in range(2):
        rr = slice(b * GROUP, (b + 1) * GROUP)
        raw = acc[rr, CONV:WIDE] + small[0:1, :]
        dt = jnp.maximum(raw, 0.0) + jnp.log1p(jnp.exp(-jnp.abs(raw)))
        ld = -dt * small[8:9, :]
        cum = lax.dot_general(
            tri, ld, (((1,), (0,)), ((), ())), precision=lax.Precision.HIGHEST, preferred_element_type=F32
        )
        cum_s[rr, :] = cum
        dt_s[rr, :] = dt
    ends = jnp.concatenate([cum_s[GROUP - 1 : GROUP, :], cum_s[ROWS - 1 : ROWS, :]], axis=0)
    total = ends[0:1, :] + ends[1:2, :]
    row8 = lax.broadcasted_iota(jnp.int32, (8, ST), 0)
    t_send[...] = jnp.where(row8 == z, total, 0.0)

    def tcopy(k):
        return remote(t_send, t_recv.at[z], ts_sem.at[k], tr_sem.at[z], seq=y * 8 + (z + k) % 8)

    for k in range(1, 8):
        tcopy(k).start()
        sent.append(tcopy(k))
    t_recv[z] = t_send[...]

    def conv(b):
        def body(j, carry):
            cols = pl.ds(pl.multiple_of(j * 128, 128), 128)

            def taps(ref, kcols):
                total = mx[pl.ds(b * GROUP + 5, GROUP), cols] * ref[0:1, kcols]
                for k in range(1, 4):
                    total = total + mx[pl.ds(b * GROUP + 5 + k, GROUP), cols] * ref[k : k + 1, kcols]
                return silu(total).astype(BF16)

            act[pl.ds(b * GROUP, GROUP), cols] = taps(kern, cols)
            return carry

        lax.fori_loop(0, CONV // 128, body, 0)

    loads[4].wait()
    loads[5].wait()

    def contribution(b):
        rr = slice(b * GROUP, (b + 1) * GROUP)
        ending = cum_s[(b + 1) * GROUP - 1 : (b + 1) * GROUP, :]
        tail = jnp.exp(ending - cum_s[rr, :]) * dt_s[rr, :]
        scaled = (act[rr, 0:CH].astype(F32) * expanded(tail)).astype(BF16)
        inject_t = act[rr, CH : CH + ST].astype(F32).T.astype(BF16)
        return dot(inject_t, scaled)

    phase("conv1")
    conv(1)
    phase("contrib1")
    c1 = contribution(1)
    st_f[...] = c1
    phase("edge_wait")
    edge.wait_recv()
    halo = edge_r[8:16, :].astype(F32)
    mx[0:8, :] = jnp.where(seq == 0, 0.0, halo)
    phase("conv0")
    conv(0)
    phase("contrib0")
    c0_s[...] = contribution(0)
    ends8 = jnp.concatenate([ends, jnp.zeros((6, ST), F32)], axis=0)
    end_exp = expanded(jnp.exp(ends8))
    st_bf[...] = (end_exp[1:2, :] * c0_s[...] + st_f[...]).astype(BF16)
    phase("zsend")
    def zcopy(k):
        to = (z + k) % 8
        return remote(st_bf.at[pl.ds(pl.multiple_of(16 * to, 16), 16), :], z_recv.at[z], zs_sem.at[k], zr_sem.at[z],
                      seq=y * 8 + to)

    for k in (4, 3, 5, 2, 6, 1, 7):
        zcopy(k).start()
        sent.append(zcopy(k))
    z_recv[z] = st_bf[pl.ds(pl.multiple_of(16 * z, 16), 16), :]

    phase("late_steps")
    for b in range(2):
        rr = slice(b * GROUP, (b + 1) * GROUP)
        cumt_s[b] = (cum_s[rr, :] * LOG2E).T[0:16, :]
        dtt_s[b] = dt_s[rr, :].T[0:16, :]
        gexp[rr, :] = expanded(jnp.exp(cum_s[rr, :]))

    def intra(b, rr0):
        t0 = pl.ds(rr0, 128)
        t1 = pl.ds(rr0 + 128, 128)
        both = pl.ds(rr0, GROUP)
        inject = act[both, CH : CH + ST]
        sc0 = dot_nt(act[t0, CH + ST : CONV], inject[0:128, :])
        sc1 = dot_nt(act[t1, CH + ST : CONV], inject)
        diag = lax.broadcasted_iota(jnp.int32, (128, 128), 0) >= lax.broadcasted_iota(jnp.int32, (128, 128), 1)
        lane = lax.broadcasted_iota(jnp.int32, (128, 128), 1) < 64
        ca = cum_s[t0, :] * LOG2E
        cb = cum_s[t1, :] * LOG2E
        for p in range(HD // 2):
            cols = slice(p * 128, (p + 1) * 128)
            chan = act[both, cols]
            res0, res1 = [], []
            for h in (2 * p, 2 * p + 1):
                ct = cumt_s[b, h : h + 1, :]
                dtr = dtt_s[b, h : h + 1, :]
                g0 = jnp.where(diag, ca[:, h : h + 1] - ct[:, 0:128], -1e30)
                m0 = (sc0 * jnp.exp2(g0) * dtr[:, 0:128]).astype(BF16)
                res0.append(dot(m0, chan[0:128, :]))
                g1 = cb[:, h : h + 1] - ct[:, 0:128]
                m1 = (sc1[:, 0:128] * jnp.exp2(g1) * dtr[:, 0:128]).astype(BF16)
                g2 = jnp.where(diag, cb[:, h : h + 1] - ct[:, 128:256], -1e30)
                m2 = (sc1[:, 128:256] * jnp.exp2(g2) * dtr[:, 128:256]).astype(BF16)
                res1.append(dot(m1, chan[0:128, :]) + dot(m2, chan[128:256, :]))
            ssd[t0, cols] = jnp.where(lane, res0[0], res0[1])
            ssd[t1, cols] = jnp.where(lane, res1[0], res1[1])

    def intra_body(b, carry):
        intra(b, pl.multiple_of(b * GROUP, GROUP))
        return carry

    phase("intra")
    lax.fori_loop(0, 2, intra_body, 0)

    phase("zwait")
    for k in range(1, 8):
        src = (z + k) % 8
        remote(st_bf.at[0:16, :], z_recv.at[src], zs_sem.at[k], zr_sem.at[src], seq=prv).wait_recv()
        remote(t_send, t_recv.at[src], ts_sem.at[k], tr_sem.at[src], seq=prv).wait_recv()
    phase("prefix")
    tall = t_recv[0]
    for k in range(1, 8):
        tall = tall + t_recv[k]
    texp = expanded(jnp.exp(tall))
    prefix = jnp.zeros((16, CH), F32)
    tsum = jnp.zeros((1, ST), F32)
    tpre = []
    for k in range(8):
        f_pre = prefix
        pref[16 * k : 16 * (k + 1), 0:CH] = f_pre
        tpre.append(tsum)
        prefix = texp[k : k + 1, :] * prefix + z_recv[k].astype(F32)
        tsum = tsum + tall[k : k + 1, :]
    y_send[...] = prefix.astype(BF16)
    yt_send[...] = jnp.where(row8 == y, tsum, 0.0)
    for k in range(1, 4):
        to = ((y + k) % 4) * 8 + z
        a = remote(y_send, y_recv.at[y], ys_sem.at[k], yr_sem.at[y], seq=to)
        b = remote(yt_send, yt_recv.at[y], yts_sem.at[k], ytr_sem.at[y], seq=to)
        for copy in (a, b):
            copy.start()
            sent.append(copy)
    y_recv[y] = y_send[...]
    yt_recv[y] = yt_send[...]

    phase("gate")
    loads[10].wait()

    def gate_body(half, carry):
        rr = pl.ds(pl.multiple_of(half * GROUP, GROUP), GROUP)
        v = dot(xb[0, rr, :], wg[0:KD, :])
        for src in range(1, 8):
            v = v + dot(xb[src, rr, :], wg[src * KD : (src + 1) * KD, :])
        acc_g[rr, :] = silu(v.astype(BF16).astype(F32))
        return carry

    lax.fori_loop(0, 2, gate_body, 0)
    phase("ywait")

    for k in range(1, 4):
        src = (y + k) % 4
        remote(y_send, y_recv.at[src], ys_sem.at[k], yr_sem.at[src], seq=prv).wait_recv()
        remote(yt_send, yt_recv.at[src], yts_sem.at[k], ytr_sem.at[src], seq=prv).wait_recv()
    phase("ycomb")
    yall = yt_recv[0]
    for k in range(1, 4):
        yall = yall + yt_recv[k]
    yexp = expanded(jnp.exp(yall))
    run = jnp.zeros((16, CH), F32)
    chosen = run
    for k in range(3):
        run = yexp[k : k + 1, :] * run + y_recv[k].astype(F32)
        chosen = jnp.where(y == k + 1, run, chosen)
    pexp = expanded(jnp.exp(jnp.concatenate(tpre, axis=0)))
    for k in range(8):
        f_send[k] = (pref[16 * k : 16 * (k + 1), 0:CH] + pexp[k : k + 1, :] * chosen).astype(BF16)
    mine = pl.ds(pl.multiple_of(16 * z, 16), 16)
    for k in (4, 3, 5, 2, 6, 1, 7):
        to = (z + k) % 8
        copy = remote(f_send.at[to], inc.at[mine, :], fs_sem.at[k], fr_sem.at[z], seq=y * 8 + to)
        copy.start()
        sent.append(copy)
    inc[mine, :] = f_send[z]

    phase("skip")
    skips = expanded(small[16:24, :])[0:1, :]
    ssd[...] = ssd[...] + skips * act[:, 0:CH].astype(F32)
    loads[9].wait()
    loads[11].wait()
    phase("fwait")

    for k in range(1, 8):
        src = (z + k) % 8
        there = pl.ds(pl.multiple_of(16 * src, 16), 16)
        remote(f_send.at[0], inc.at[there, :], fs_sem.at[k], fr_sem.at[src], seq=prv).wait_recv()
    phase("gated")
    carr[0] = inc[...]
    carr[1] = (c0_s[...] + end_exp[0:1, :] * inc[...].astype(F32)).astype(BF16)

    ones = jnp.ones((8, CH), BF16)
    gain_row = gain_v[...].reshape(1, CH)

    def gate(chip):
        rr = pl.ds(pl.multiple_of(chip * 128, 128), 128)
        reads = dot(act[rr, CH + ST : CONV], carr[chip // 2])
        g = (ssd[rr, :] + reads * gexp[rr, :]) * acc_g[rr, :]
        hi, lo = split2(g * g)
        sq_send[chip] = dot_nt(ones, hi) + dot_nt(ones, lo)
        return (g * gain_row).astype(BF16)

    def started(copy):
        copy.start()
        sent.append(copy)

    def part(ref, *at):
        return ref.at[at + (slice(None), pl.ds(0, CUTS[at[-1]][1]))]

    def dcopy(j, q):
        return remote(part(d_send, j, q), part(d_recv, j, q), ds_sem.at[j, q], dr_sem.at[j, q], tp=partner)

    def project(j, rows):
        for q, (start, width) in enumerate(CUTS):
            cols = pl.ds(0, width)
            v = dot(rows, wo[:, start : start + width])
            both[0, :, cols] = v[0:64, :]
            both[1, :, cols] = v[64:128, :]
            d_send[j, q, :, cols] = both[1 - c, :, cols].astype(BF16)
            started(dcopy(j, q))
            keep[j, q, :, cols] = both[c, :, cols]

    def paired(j, q):
        dcopy(j, q).wait_recv()
        cols = pl.ds(0, CUTS[q][1])
        return keep[j, q, :, cols] + d_recv[j, q, :, cols].astype(F32)

    def hop1(q):
        to = right if q % 2 == 0 else left
        return remote(part(r1_send, 0, q), part(r1_recv, q), rs_sem.at[q, 0], rr_sem.at[q, 0], tp=to)

    def direct(q):
        if q % 2 == 0:
            return remote(part(r1_send, 1, q), part(fin_r, q), rs_sem.at[q, 1], rr_sem.at[q, 1], tp=left)
        return remote(part(r1_send, 1, q), part(fin_l, q), rs_sem.at[q, 1], rr_sem.at[q, 1], tp=right)

    def hop2(q):
        if q % 2 == 0:
            return remote(part(r1_send, 2, q), part(fin_l, q), rs_sem.at[q, 2], rr_sem.at[q, 2], tp=right)
        return remote(part(r1_send, 2, q), part(fin_r, q), rs_sem.at[q, 2], rr_sem.at[q, 2], tp=left)

    def put(which, q, value):
        r1_send[which, q, :, pl.ds(0, CUTS[q][1])] = value.astype(BF16)

    project(0, gate(ox))
    phase("block1")
    rows = gate(lx)
    phase("hop1")
    for q in range(NQ):
        put(0, q, paired(0, q))
        started(hop1(q))
    phase("block1_mm")
    project(1, rows)
    phase("block2")
    project(2, gate(rx))
    phase("direct")
    for q in range(NQ):
        put(1, q, paired(1 if q % 2 == 0 else 2, q))
        started(direct(q))
    phase("block3")
    project(3, gate(x))
    for k in range(1, 8):
        to = (tp + k) % 8
        started(remote(sq_send.at[to // 2], sq_recv.at[tp], qs_sem.at[k], qr_sem.at[tp], tp=to))
    sq_recv[tp] = sq_send[x]
    phase("hop2")
    for q in range(NQ):
        v = paired(2 if q % 2 == 0 else 1, q)
        hop1(q).wait_recv()
        put(2, q, v + r1_recv[q, :, pl.ds(0, CUTS[q][1])].astype(F32))
        started(hop2(q))
    phase("own_sum")
    for q in range(NQ):
        keep[3, q, :, pl.ds(0, CUTS[q][1])] = paired(3, q)
    phase("scale")
    for k in range(1, 8):
        src = (tp + k) % 8
        remote(sq_send.at[0], sq_recv.at[src], qs_sem.at[k], qr_sem.at[src], tp=partner).wait_recv()
    sq = sq_recv[0]
    for k in range(1, 8):
        sq = sq + sq_recv[k]
    factor = lax.rsqrt(sq * (1.0 / INNER) + 1e-5)
    scale_s[...] = jnp.broadcast_to(factor[0:1, :], (128, 128)).T
    scale = scale_s[pl.ds(pl.multiple_of(64 * c, 64), 64), :]
    for q, (start, width) in enumerate(CUTS):
        direct(q).wait_recv()
        hop2(q).wait_recv()
        for j in range(width // 128):
            cols = slice(j * 128, (j + 1) * 128)
            v = keep[3, q, :, cols] + fin_l[q, :, cols].astype(F32) + fin_r[q, :, cols].astype(F32)
            out[:, start + j * 128 : start + (j + 1) * 128] = (v * scale).astype(BF16)
    phase("drain")
    edge.wait_send()
    for copy in sent:
        copy.wait_send()
    phase.close()


def on_device(tok, w_gate, w_inner, w_state, w_step, k_inner, k_state, bias, rate, skip, gain, w_out):
    vm = pltpu.VMEM
    dma = pltpu.SemaphoreType.DMA
    scratch = [
        vm((8, ROWS, KD), BF16), vm((KD, ROWS), BF16), vm((HD, D), BF16), vm((ST, D), F32), vm((D, CH), BF16), vm((D, WIDE), BF16),
        vm((CH, D), BF16), vm((4, CONV), F32), vm((3, HD), F32), vm((CH,), F32),
        vm((ROWS, WIDE), F32), vm((ROWS, CH), F32),
        vm((8 + ROWS, CONV), F32), vm((ROWS, CONV), BF16), vm((16, CONV), BF16), vm((16, CONV), BF16),
        vm((24, ST), F32), vm((ST, CH), BF16), vm((ROWS, ST), F32), vm((ROWS, ST), F32),
        vm((2, 16, GROUP), F32), vm((2, 16, GROUP), F32),
        vm((ROWS, CH), F32), vm((ROWS, CH), F32), vm((ST, CH), BF16), vm((ST, CH), F32), vm((ST, CH), F32),
        vm((8, 16, CH), BF16), vm((8, ST), F32), vm((8, 8, ST), F32), vm((ST, CONV), F32),
        vm((16, CH), BF16), vm((8, ST), F32), vm((4, 16, CH), BF16), vm((4, 8, ST), F32),
        vm((8, 16, CH), BF16), vm((ST, CH), BF16), vm((2, ST, CH), BF16),
        vm((4, 8, ST), F32), vm((8, 8, ST), F32), vm((2, 64, QC), F32),
        vm((4, NQ, 64, QC), F32), vm((4, NQ, 64, QC), BF16), vm((4, NQ, 64, QC), BF16),
        vm((3, NQ, 64, QC), BF16), vm((NQ, 64, QC), BF16),
        vm((NQ, 64, QC), BF16), vm((NQ, 64, QC), BF16), vm((128, 128), F32),
        dma((12,)), dma((14,)), dma((8, 2)), dma((2,)), dma((8,)), dma((8,)), dma((8,)), dma((8,)),
        dma((4,)), dma((4,)), dma((4,)), dma((4,)), dma((8,)), dma((8,)),
        dma((8,)), dma((8,)), dma((4, NQ)), dma((4, NQ)), dma((NQ, 3)), dma((NQ, 3)),
    ]
    hbm = pl.BlockSpec(memory_space=pl.ANY)
    local = pl.BlockSpec(memory_space=pltpu.VMEM)
    return pl.pallas_call(
        kernel,
        name="layer",
        out_shape=jax.ShapeDtypeStruct((ROWS // 8, D), BF16),
        in_specs=[hbm] * 12,
        out_specs=local,
        scratch_shapes=scratch,
        compiler_params=pltpu.CompilerParams(
            collective_id=0, has_side_effects=True, vmem_limit_bytes=62 * 1024 * 1024
        ),
    )(
        tok.T, w_gate, w_inner, w_state, w_step.T, k_inner, k_state,
        bias.reshape(1, -1), rate.reshape(1, -1), skip.reshape(1, -1), gain, w_out,
    )


def solution(mesh):
    return jax.shard_map(
        on_device,
        mesh=mesh,
        in_specs=(
            P("seq", "tp"), P(None, "tp"), P(None, "tp"), P(), P(None, "tp"), P(None, "tp"), P(),
            P("tp"), P("tp"), P("tp"), P("tp"), P("tp", None),
        ),
        out_specs=P(("seq", "tp"), None),
        check_vma=False,
    )
```

```python
import jax
import jax.numpy as jnp
from jax import lax
from jax.experimental import pallas as pl
from jax.experimental.pallas import tpu as pltpu
from jax.sharding import PartitionSpec as P

MESH = pl.DeviceIdType.MESH
F32 = jnp.float32
BF16 = jnp.bfloat16
ROWS = 512
GROUP = 256
KD = 320
D = 2560
CH = 640
HD = 10
ST = 128
CONV = CH + 2 * ST
WIDE = CONV + ST
CUTS = ((0, 512), (1280, 512), (512, 768), (1792, 768))
NQ = len(CUTS)
PIECES = ((0, 112), (112, 128), (240, 144), (384, 128))
EARLY = 240
QC = 768
LOG2E = 1.4426950408889634
INNER = 5120


def split2(v):
    hi = v.astype(BF16)
    return hi, (v - hi.astype(F32)).astype(BF16)


def dot(a, b):
    return jnp.dot(a, b, preferred_element_type=F32)


def dot_nt(a, b):
    return lax.dot_general(a, b, (((1,), (1,)), ((), ())), preferred_element_type=F32)


class Phases:
    open_scope = None

    def __call__(self, name):
        self.close()
        self.open_scope = jax.named_scope(name)
        self.open_scope.__enter__()

    def close(self):
        if self.open_scope is not None:
            self.open_scope.__exit__(None, None, None)
            self.open_scope = None


def silu(v):
    return 0.5 * v * (1.0 + jnp.tanh(0.5 * v))


def kernel(
    tok, w_gate, w_inner, w_state, w_step, k_inner, k_state, bias, rate, skip, gain, w_out,
    out,
    xb, tok_t, step_t, step_f, wg, wall, wo, kern, vec, gain_v,
    acc, acc_g, mx, act, edge_s, edge_r,
    small, expand, cum_s, dt_s, cumt_s, dtt_s,
    ssd, gexp, st_bf, st_f, c0_s, z_recv, t_send, t_recv, pref, y_send, yt_send, y_recv, yt_recv, f_send, inc, carr,
    sq_send, sq_recv, both, keep, d_send, d_recv, r1_send, r1_recv, fin_l, fin_r, scale_s,
    loc_sem, g_send, g_recv, e_sem, zs_sem, zr_sem, ts_sem, tr_sem, ys_sem, yr_sem, yts_sem, ytr_sem, fs_sem, fr_sem,
    qs_sem, qr_sem, ds_sem, dr_sem, rs_sem, rr_sem,
):
    seq = lax.axis_index("seq")
    tp = lax.axis_index("tp")
    x = tp // 2
    c = tp % 2
    y = seq // 8
    z = seq % 8
    partner = 2 * x + (1 - c)
    rx, lx, ox = (x + 1) % 4, (x + 3) % 4, (x + 2) % 4
    right, left, opp = 2 * rx + c, 2 * lx + c, 2 * ox + c
    nxt, prv = (seq + 1) % 32, (seq + 31) % 32

    def remote(src, dst, ssem, rsem, **where):
        return pltpu.make_async_remote_copy(
            src_ref=src, dst_ref=dst, send_sem=ssem, recv_sem=rsem, device_id=where, device_id_type=MESH
        )

    phase = Phases()
    phase("start")
    copies = (
        (tok, tok_t), (w_inner, wall.at[:, 0:CH]), (w_state, wall.at[:, CH:CONV]), (w_step, step_t),
        (k_inner, kern.at[:, 0:CH]), (k_state, kern.at[:, CH:CONV]), (bias, vec.at[0:1]), (rate, vec.at[1:2]),
        (skip, vec.at[2:3]), (gain, gain_v), (w_gate, wg), (w_out, wo),
    )
    loads = [pltpu.make_async_copy(src, dst, loc_sem.at[i]) for i, (src, dst) in enumerate(copies)]
    for load in loads:
        load.start()

    barrier = pltpu.get_barrier_semaphore()
    for k in range(1, 8):
        pl.semaphore_signal(barrier, inc=1, device_id={"tp": (tp + k) % 8}, device_id_type=MESH)
    for k in range(1, 8):
        pl.semaphore_signal(barrier, inc=1, device_id={"seq": y * 8 + (z + k) % 8}, device_id_type=MESH)
    for k in range(1, 4):
        pl.semaphore_signal(barrier, inc=1, device_id={"seq": ((y + k) % 4) * 8 + z}, device_id_type=MESH)
    for s in (nxt, prv):
        pl.semaphore_signal(barrier, inc=1, device_id={"seq": s}, device_id_type=MESH)

    er = lax.broadcasted_iota(jnp.int32, (ST, CH), 0)
    ec = lax.broadcasted_iota(jnp.int32, (ST, CH), 1)
    off = ec - er * 64
    expand[...] = jnp.where((off >= 0) & (off < 64), 1.0, 0.0).astype(BF16)
    small[...] = jnp.zeros_like(small)

    def expanded(v):
        hi, lo = split2(v)
        return dot(hi, expand[...]) + dot(lo, expand[...])

    phase("turn")
    loads[0].wait()
    xb[tp] = tok_t[...].T
    phase("barrier")
    pl.semaphore_wait(barrier, 19)

    phase("send")
    sent = []

    def piece(src, q, to, ssem):
        start, rows = PIECES[q]
        part = xb.at[src, pl.ds(start, rows), :]
        return remote(part, part, ssem, g_recv.at[src, q], tp=to)

    gathered = []

    def send(src, q, to):
        copy = piece(src, q, to, g_send.at[len(gathered)])
        copy.start()
        gathered.append(copy)
        sent.append(copy)

    def arrived(src, q):
        piece(src, q, partner, g_send.at[0]).wait_recv()

    for a, b in ((2, 3), (3, 2), (0, 1)):
        send(tp, a, right)
        send(tp, b, left)
    for q in (2, 3, 0, 1):
        send(tp, q, partner)
    phase("step_turn")
    loads[3].wait()
    step_f[...] = jnp.zeros_like(step_f)
    step_f[0:HD, :] = step_t[...].astype(F32)
    wall[:, CONV:WIDE] = step_f[...].T.astype(BF16)
    for i in (6, 7, 8):
        loads[i].wait()
        small[8 * (i - 6) : 8 * (i - 6) + 1, 0:HD] = vec[i - 6 : i - 5, :]
    loads[1].wait()
    loads[2].wait()

    def accumulate(src, start, rows, first=False):
        rr = pl.ds(start, rows)
        v = dot(xb[src, rr, :], wall[pl.ds(pl.multiple_of(src * KD, 64), KD), :])
        acc[rr, :] = v if first else acc[rr, :] + v

    early, late = (EARLY, ROWS - EARLY), (0, EARLY)
    rp, lp, op = 2 * rx + 1 - c, 2 * lx + 1 - c, 2 * ox + 1 - c
    phase("own")
    accumulate(tp, *early, True)
    accumulate(tp, *late, True)
    for q in (2, 3):
        arrived(partner, q)
    accumulate(partner, *early)
    for q in (0, 1):
        arrived(partner, q)
    accumulate(partner, *late)
    phase("near0")
    arrived(left, 2)
    send(left, 2, right)
    send(left, 2, partner)
    send(tp, 1, right)
    arrived(right, 3)
    send(right, 3, left)
    send(right, 3, partner)
    send(tp, 0, left)
    phase("near1")
    arrived(left, 3)
    send(left, 3, partner)
    arrived(right, 2)
    send(right, 2, partner)
    phase("near_early")
    accumulate(left, *early)
    accumulate(right, *early)
    phase("near2")
    arrived(left, 0)
    send(left, 0, right)
    send(left, 0, partner)
    arrived(right, 1)
    send(right, 1, left)
    send(right, 1, partner)
    phase("nearp_early")
    for src in (lp, rp):
        arrived(src, 2)
        arrived(src, 3)
        accumulate(src, *early)
    phase("far_early")
    for q in (2, 3):
        arrived(opp, q)
        send(opp, q, partner)
    accumulate(opp, *early)
    phase("farp_early")
    for q in (2, 3):
        arrived(op, q)
    accumulate(op, *early)

    phase("edge")
    edge_s[...] = acc[ROWS - 16 : ROWS, 0:CONV].astype(BF16)
    edge = remote(edge_s, edge_r, e_sem.at[0], e_sem.at[1], seq=nxt)
    edge.start()
    mx[8 + EARLY : 8 + ROWS, :] = acc[EARLY:ROWS, 0:CONV].astype(BF16).astype(F32)

    tri = (
        lax.broadcasted_iota(jnp.int32, (GROUP, GROUP), 0) >= lax.broadcasted_iota(jnp.int32, (GROUP, GROUP), 1)
    ).astype(F32)

    def steps(b):
        rr = slice(b * GROUP, (b + 1) * GROUP)
        raw = acc[rr, CONV:WIDE] + small[0:1, :]
        dt = jnp.maximum(raw, 0.0) + jnp.log1p(jnp.exp(-jnp.abs(raw)))
        ld = -dt * small[8:9, :]
        cum = lax.dot_general(
            tri, ld, (((1,), (0,)), ((), ())), precision=lax.Precision.HIGHEST, preferred_element_type=F32
        )
        cum_s[rr, :] = cum
        dt_s[rr, :] = dt

    def conv(b, first=0, last=CONV // 128 - 1):
        def body(j, carry):
            cols = pl.ds(pl.multiple_of(j * 128, 128), 128)

            def taps(ref, kcols):
                total = mx[pl.ds(b * GROUP + 5, GROUP), cols] * ref[0:1, kcols]
                for k in range(1, 4):
                    total = total + mx[pl.ds(b * GROUP + 5 + k, GROUP), cols] * ref[k : k + 1, kcols]
                return silu(total).astype(BF16)

            act[pl.ds(b * GROUP, GROUP), cols] = taps(kern, cols)
            return carry

        lax.fori_loop(first, last, body, 0)

    loads[4].wait()
    loads[5].wait()

    def contribution(b):
        rr = slice(b * GROUP, (b + 1) * GROUP)
        ending = cum_s[(b + 1) * GROUP - 1 : (b + 1) * GROUP, :]
        tail = jnp.exp(ending - cum_s[rr, :]) * dt_s[rr, :]
        scaled = (act[rr, 0:CH].astype(F32) * expanded(tail)).astype(BF16)
        inject_t = act[rr, CH : CH + ST].astype(F32).T.astype(BF16)
        return dot(inject_t, scaled)

    phase("steps1")
    steps(1)
    phase("conv1")
    conv(1)
    phase("near3")
    arrived(left, 1)
    send(left, 1, partner)
    arrived(right, 0)
    send(right, 0, partner)
    accumulate(left, *late)
    accumulate(right, *late)
    phase("contrib1")
    st_f[...] = contribution(1)
    phase("far_late")
    for q in (0, 1):
        arrived(opp, q)
        send(opp, q, partner)
    for src in (lp, rp):
        arrived(src, 0)
        arrived(src, 1)
        accumulate(src, *late)
    accumulate(opp, *late)
    phase("farp_late")
    for q in (0, 1):
        arrived(op, q)
    accumulate(op, *late)
    mx[8 : 8 + EARLY, :] = acc[0:EARLY, 0:CONV].astype(BF16).astype(F32)
    phase("steps0")
    steps(0)
    ends = jnp.concatenate([cum_s[GROUP - 1 : GROUP, :], cum_s[ROWS - 1 : ROWS, :]], axis=0)
    total = ends[0:1, :] + ends[1:2, :]
    row8 = lax.broadcasted_iota(jnp.int32, (8, ST), 0)
    t_send[...] = jnp.where(row8 == z, total, 0.0)

    def tcopy(k):
        return remote(t_send, t_recv.at[z], ts_sem.at[k], tr_sem.at[z], seq=y * 8 + (z + k) % 8)

    for k in range(1, 8):
        tcopy(k).start()
        sent.append(tcopy(k))
    t_recv[z] = t_send[...]

    phase("edge_wait")
    edge.wait_recv()
    halo = edge_r[8:16, :].astype(F32)
    mx[0:8, :] = jnp.where(seq == 0, 0.0, halo)
    phase("conv0")
    conv(0)
    phase("contrib0")
    c0_s[...] = contribution(0)
    ends8 = jnp.concatenate([ends, jnp.zeros((6, ST), F32)], axis=0)
    end_exp = expanded(jnp.exp(ends8))
    st_bf[...] = (end_exp[1:2, :] * c0_s[...] + st_f[...]).astype(BF16)
    phase("zsend")
    def zcopy(k):
        to = (z + k) % 8
        return remote(st_bf.at[pl.ds(pl.multiple_of(16 * to, 16), 16), :], z_recv.at[z], zs_sem.at[k], zr_sem.at[z],
                      seq=y * 8 + to)

    for k in (4, 3, 5, 2, 6, 1, 7):
        zcopy(k).start()
        sent.append(zcopy(k))
    z_recv[z] = st_bf[pl.ds(pl.multiple_of(16 * z, 16), 16), :]

    phase("late_steps")
    for b in range(2):
        conv(b, CONV // 128 - 1, CONV // 128)
    for b in range(2):
        rr = slice(b * GROUP, (b + 1) * GROUP)
        cumt_s[b] = (cum_s[rr, :] * LOG2E).T[0:16, :]
        dtt_s[b] = dt_s[rr, :].T[0:16, :]
        gexp[rr, :] = expanded(jnp.exp(cum_s[rr, :]))

    def intra(b, rr0):
        t0 = pl.ds(rr0, 128)
        t1 = pl.ds(rr0 + 128, 128)
        both = pl.ds(rr0, GROUP)
        inject = act[both, CH : CH + ST]
        sc0 = dot_nt(act[t0, CH + ST : CONV], inject[0:128, :])
        sc1 = dot_nt(act[t1, CH + ST : CONV], inject)
        diag = lax.broadcasted_iota(jnp.int32, (128, 128), 0) >= lax.broadcasted_iota(jnp.int32, (128, 128), 1)
        lane = lax.broadcasted_iota(jnp.int32, (128, 128), 1) < 64
        ca = cum_s[t0, :] * LOG2E
        cb = cum_s[t1, :] * LOG2E
        for p in range(HD // 2):
            cols = slice(p * 128, (p + 1) * 128)
            chan = act[both, cols]
            res0, res1 = [], []
            for h in (2 * p, 2 * p + 1):
                ct = cumt_s[b, h : h + 1, :]
                dtr = dtt_s[b, h : h + 1, :]
                g0 = jnp.where(diag, ca[:, h : h + 1] - ct[:, 0:128], -1e30)
                m0 = (sc0 * jnp.exp2(g0) * dtr[:, 0:128]).astype(BF16)
                res0.append(dot(m0, chan[0:128, :]))
                g1 = cb[:, h : h + 1] - ct[:, 0:128]
                m1 = (sc1[:, 0:128] * jnp.exp2(g1) * dtr[:, 0:128]).astype(BF16)
                g2 = jnp.where(diag, cb[:, h : h + 1] - ct[:, 128:256], -1e30)
                m2 = (sc1[:, 128:256] * jnp.exp2(g2) * dtr[:, 128:256]).astype(BF16)
                res1.append(dot(m1, chan[0:128, :]) + dot(m2, chan[128:256, :]))
            ssd[t0, cols] = jnp.where(lane, res0[0], res0[1])
            ssd[t1, cols] = jnp.where(lane, res1[0], res1[1])

    def intra_body(b, carry):
        intra(b, pl.multiple_of(b * GROUP, GROUP))
        return carry

    phase("intra")
    lax.fori_loop(0, 2, intra_body, 0)

    phase("decays")
    for k in range(1, 8):
        src = (z + k) % 8
        remote(t_send, t_recv.at[src], ts_sem.at[k], tr_sem.at[src], seq=prv).wait_recv()
    tall = t_recv[0]
    for k in range(1, 8):
        tall = tall + t_recv[k]
    texp = expanded(jnp.exp(tall))
    tsum = jnp.zeros((1, ST), F32)
    tpre = []
    for k in range(8):
        tpre.append(tsum)
        tsum = tsum + tall[k : k + 1, :]
    pexp = expanded(jnp.exp(jnp.concatenate(tpre, axis=0)))
    yt_send[...] = jnp.where(row8 == y, tsum, 0.0)
    for k in range(1, 4):
        to = ((y + k) % 4) * 8 + z
        copy = remote(yt_send, yt_recv.at[y], yts_sem.at[k], ytr_sem.at[y], seq=to)
        copy.start()
        sent.append(copy)
    yt_recv[y] = yt_send[...]

    phase("gate0")
    loads[10].wait()

    def gate_half(half):
        rr = slice(half * GROUP, (half + 1) * GROUP)
        v = dot(xb[0, rr, :], wg[0:KD, :])
        for src in range(1, 8):
            v = v + dot(xb[src, rr, :], wg[src * KD : (src + 1) * KD, :])
        acc_g[rr, :] = silu(v.astype(BF16).astype(F32))

    gate_half(0)

    phase("zwait")
    for k in range(1, 8):
        src = (z + k) % 8
        remote(st_bf.at[0:16, :], z_recv.at[src], zs_sem.at[k], zr_sem.at[src], seq=prv).wait_recv()
    phase("prefix")
    prefix = jnp.zeros((16, CH), F32)
    for k in range(8):
        pref[16 * k : 16 * (k + 1), 0:CH] = prefix
        prefix = texp[k : k + 1, :] * prefix + z_recv[k].astype(F32)
    y_send[...] = prefix.astype(BF16)
    for k in (2, 1, 3):
        to = ((y + k) % 4) * 8 + z
        copy = remote(y_send, y_recv.at[y], ys_sem.at[k], yr_sem.at[y], seq=to)
        copy.start()
        sent.append(copy)
    y_recv[y] = y_send[...]

    phase("gate1")
    gate_half(1)
    phase("ywait")
    for k in range(1, 4):
        src = (y + k) % 4
        remote(yt_send, yt_recv.at[src], yts_sem.at[k], ytr_sem.at[src], seq=prv).wait_recv()
    yall = yt_recv[0]
    for k in range(1, 4):
        yall = yall + yt_recv[k]
    yexp = expanded(jnp.exp(yall))
    for k in range(1, 4):
        src = (y + k) % 4
        remote(y_send, y_recv.at[src], ys_sem.at[k], yr_sem.at[src], seq=prv).wait_recv()
    phase("ycomb")
    run = jnp.zeros((16, CH), F32)
    chosen = run
    for k in range(3):
        run = yexp[k : k + 1, :] * run + y_recv[k].astype(F32)
        chosen = jnp.where(y == k + 1, run, chosen)
    for k in range(8):
        f_send[k] = (pref[16 * k : 16 * (k + 1), 0:CH] + pexp[k : k + 1, :] * chosen).astype(BF16)
    mine = pl.ds(pl.multiple_of(16 * z, 16), 16)
    for k in (4, 3, 5, 2, 6, 1, 7):
        to = (z + k) % 8
        copy = remote(f_send.at[to], inc.at[mine, :], fs_sem.at[k], fr_sem.at[z], seq=y * 8 + to)
        copy.start()
        sent.append(copy)
    inc[mine, :] = f_send[z]

    phase("skip")
    skips = expanded(small[16:24, :])[0:1, :]
    ssd[...] = ssd[...] + skips * act[:, 0:CH].astype(F32)
    loads[9].wait()
    loads[11].wait()
    phase("fwait")

    for k in range(1, 8):
        src = (z + k) % 8
        there = pl.ds(pl.multiple_of(16 * src, 16), 16)
        remote(f_send.at[0], inc.at[there, :], fs_sem.at[k], fr_sem.at[src], seq=prv).wait_recv()
    phase("gated")
    carr[0] = inc[...]
    carr[1] = (c0_s[...] + end_exp[0:1, :] * inc[...].astype(F32)).astype(BF16)

    ones = jnp.ones((8, CH), BF16)
    gain_row = gain_v[...].reshape(1, CH)

    def gate(chip):
        rr = pl.ds(pl.multiple_of(chip * 128, 128), 128)
        reads = dot(act[rr, CH + ST : CONV], carr[chip // 2])
        g = (ssd[rr, :] + reads * gexp[rr, :]) * acc_g[rr, :]
        hi, lo = split2(g * g)
        sq_send[chip] = dot_nt(ones, hi) + dot_nt(ones, lo)
        return (g * gain_row).astype(BF16)

    def started(copy):
        copy.start()
        sent.append(copy)

    def part(ref, *at):
        return ref.at[at + (slice(None), pl.ds(0, CUTS[at[-1]][1]))]

    def dcopy(j, q):
        return remote(part(d_send, j, q), part(d_recv, j, q), ds_sem.at[j, q], dr_sem.at[j, q], tp=partner)

    def project(j, rows):
        for q, (start, width) in enumerate(CUTS):
            cols = pl.ds(0, width)
            v = dot(rows, wo[:, start : start + width])
            both[0, :, cols] = v[0:64, :]
            both[1, :, cols] = v[64:128, :]
            d_send[j, q, :, cols] = both[1 - c, :, cols].astype(BF16)
            started(dcopy(j, q))
            keep[j, q, :, cols] = both[c, :, cols]

    def paired(j, q):
        dcopy(j, q).wait_recv()
        cols = pl.ds(0, CUTS[q][1])
        return keep[j, q, :, cols] + d_recv[j, q, :, cols].astype(F32)

    def hop1(q):
        to = right if q % 2 == 0 else left
        return remote(part(r1_send, 0, q), part(r1_recv, q), rs_sem.at[q, 0], rr_sem.at[q, 0], tp=to)

    def direct(q):
        if q % 2 == 0:
            return remote(part(r1_send, 1, q), part(fin_r, q), rs_sem.at[q, 1], rr_sem.at[q, 1], tp=left)
        return remote(part(r1_send, 1, q), part(fin_l, q), rs_sem.at[q, 1], rr_sem.at[q, 1], tp=right)

    def hop2(q):
        if q % 2 == 0:
            return remote(part(r1_send, 2, q), part(fin_l, q), rs_sem.at[q, 2], rr_sem.at[q, 2], tp=right)
        return remote(part(r1_send, 2, q), part(fin_r, q), rs_sem.at[q, 2], rr_sem.at[q, 2], tp=left)

    def put(which, q, value):
        r1_send[which, q, :, pl.ds(0, CUTS[q][1])] = value.astype(BF16)

    project(0, gate(ox))
    phase("block1")
    rows = gate(lx)
    phase("hop1")
    for q in range(NQ):
        put(0, q, paired(0, q))
        started(hop1(q))
    phase("block1_mm")
    project(1, rows)
    phase("block2")
    project(2, gate(rx))
    phase("direct")
    for q in range(NQ):
        put(1, q, paired(1 if q % 2 == 0 else 2, q))
        started(direct(q))
    phase("block3")
    project(3, gate(x))
    for k in range(1, 8):
        to = (tp + k) % 8
        started(remote(sq_send.at[to // 2], sq_recv.at[tp], qs_sem.at[k], qr_sem.at[tp], tp=to))
    sq_recv[tp] = sq_send[x]
    phase("hop2")
    for q in range(NQ):
        v = paired(2 if q % 2 == 0 else 1, q)
        hop1(q).wait_recv()
        put(2, q, v + r1_recv[q, :, pl.ds(0, CUTS[q][1])].astype(F32))
        started(hop2(q))
    phase("own_sum")
    for q in range(NQ):
        keep[3, q, :, pl.ds(0, CUTS[q][1])] = paired(3, q)
    phase("scale")
    for k in range(1, 8):
        src = (tp + k) % 8
        remote(sq_send.at[0], sq_recv.at[src], qs_sem.at[k], qr_sem.at[src], tp=partner).wait_recv()
    sq = sq_recv[0]
    for k in range(1, 8):
        sq = sq + sq_recv[k]
    factor = lax.rsqrt(sq * (1.0 / INNER) + 1e-5)
    scale_s[...] = jnp.broadcast_to(factor[0:1, :], (128, 128)).T
    scale = scale_s[pl.ds(pl.multiple_of(64 * c, 64), 64), :]
    for q, (start, width) in enumerate(CUTS):
        direct(q).wait_recv()
        hop2(q).wait_recv()
        for j in range(width // 128):
            cols = slice(j * 128, (j + 1) * 128)
            v = keep[3, q, :, cols] + fin_l[q, :, cols].astype(F32) + fin_r[q, :, cols].astype(F32)
            out[:, start + j * 128 : start + (j + 1) * 128] = (v * scale).astype(BF16)
    phase("drain")
    edge.wait_send()
    for copy in sent:
        copy.wait_send()
    phase.close()


def on_device(tok, w_gate, w_inner, w_state, w_step, k_inner, k_state, bias, rate, skip, gain, w_out):
    vm = pltpu.VMEM
    dma = pltpu.SemaphoreType.DMA
    scratch = [
        vm((8, ROWS, KD), BF16), vm((KD, ROWS), BF16), vm((HD, D), BF16), vm((ST, D), F32), vm((D, CH), BF16), vm((D, WIDE), BF16),
        vm((CH, D), BF16), vm((4, CONV), F32), vm((3, HD), F32), vm((CH,), F32),
        vm((ROWS, WIDE), F32), vm((ROWS, CH), F32),
        vm((8 + ROWS, CONV), F32), vm((ROWS, CONV), BF16), vm((16, CONV), BF16), vm((16, CONV), BF16),
        vm((24, ST), F32), vm((ST, CH), BF16), vm((ROWS, ST), F32), vm((ROWS, ST), F32),
        vm((2, 16, GROUP), F32), vm((2, 16, GROUP), F32),
        vm((ROWS, CH), F32), vm((ROWS, CH), F32), vm((ST, CH), BF16), vm((ST, CH), F32), vm((ST, CH), F32),
        vm((8, 16, CH), BF16), vm((8, ST), F32), vm((8, 8, ST), F32), vm((ST, CONV), F32),
        vm((16, CH), BF16), vm((8, ST), F32), vm((4, 16, CH), BF16), vm((4, 8, ST), F32),
        vm((8, 16, CH), BF16), vm((ST, CH), BF16), vm((2, ST, CH), BF16),
        vm((4, 8, ST), F32), vm((8, 8, ST), F32), vm((2, 64, QC), F32),
        vm((4, NQ, 64, QC), F32), vm((4, NQ, 64, QC), BF16), vm((4, NQ, 64, QC), BF16),
        vm((3, NQ, 64, QC), BF16), vm((NQ, 64, QC), BF16),
        vm((NQ, 64, QC), BF16), vm((NQ, 64, QC), BF16), vm((128, 128), F32),
        dma((12,)), dma((28,)), dma((8, 4)), dma((2,)), dma((8,)), dma((8,)), dma((8,)), dma((8,)),
        dma((4,)), dma((4,)), dma((4,)), dma((4,)), dma((8,)), dma((8,)),
        dma((8,)), dma((8,)), dma((4, NQ)), dma((4, NQ)), dma((NQ, 3)), dma((NQ, 3)),
    ]
    hbm = pl.BlockSpec(memory_space=pl.ANY)
    local = pl.BlockSpec(memory_space=pltpu.VMEM)
    return pl.pallas_call(
        kernel,
        name="layer",
        out_shape=pltpu.VMEM((ROWS // 8, D), BF16),
        in_specs=[hbm] * 12,
        out_specs=local,
        scratch_shapes=scratch,
        compiler_params=pltpu.CompilerParams(
            collective_id=0, has_side_effects=True, vmem_limit_bytes=62 * 1024 * 1024
        ),
    )(
        tok.T, w_gate, w_inner, w_state, w_step.T, k_inner, k_state,
        bias.reshape(1, -1), rate.reshape(1, -1), skip.reshape(1, -1), gain, w_out,
    )


def solution(mesh):
    return jax.shard_map(
        on_device,
        mesh=mesh,
        in_specs=(
            P("seq", "tp"), P(None, "tp"), P(None, "tp"), P(), P(None, "tp"), P(None, "tp"), P(),
            P("tp"), P("tp"), P("tp"), P("tp"), P("tp", None),
        ),
        out_specs=P(("seq", "tp"), None),
        check_vma=False,
    )
```

```python
import jax
import jax.numpy as jnp
from jax import lax
from jax.experimental import pallas as pl
from jax.experimental.pallas import tpu as pltpu
from jax.sharding import PartitionSpec as P

MESH = pl.DeviceIdType.MESH
F32 = jnp.float32
BF16 = jnp.bfloat16
ROWS = 512
GROUP = 256
KD = 320
D = 2560
CH = 640
HD = 10
ST = 128
CONV = CH + 2 * ST
WIDE = CONV + ST
CUTS = ((0, 512), (1280, 512), (512, 768), (1792, 768))
NQ = len(CUTS)
PIECES = ((0, 112), (112, 128), (240, 144), (384, 128), (0, 240), (240, 272))
EARLY = 240
QC = 768
LOG2E = 1.4426950408889634
INNER = 5120


def split2(v):
    hi = v.astype(BF16)
    return hi, (v - hi.astype(F32)).astype(BF16)


def dot(a, b):
    return jnp.dot(a, b, preferred_element_type=F32)


def dot_nt(a, b):
    return lax.dot_general(a, b, (((1,), (1,)), ((), ())), preferred_element_type=F32)


class Phases:
    open_scope = None

    def __call__(self, name):
        self.close()
        self.open_scope = jax.named_scope(name)
        self.open_scope.__enter__()

    def close(self):
        if self.open_scope is not None:
            self.open_scope.__exit__(None, None, None)
            self.open_scope = None


def silu(v):
    return 0.5 * v * (1.0 + jnp.tanh(0.5 * v))


def kernel(
    tok, w_gate, w_inner, w_state, w_step, k_inner, k_state, bias, rate, skip, gain, w_out,
    out,
    xb, tok_t, step_t, step_f, wg, wall, wo, kern, vec, gain_v,
    acc, acc_g, mx, act, edge_s, edge_r,
    small, expand, cum_s, dt_s, cumt_s, dtt_s,
    ssd, gexp, st_bf, st_f, c0_s, z_recv, t_send, t_recv, pref, y_send, yt_send, y_recv, yt_recv, f_send, inc, carr,
    sq_send, sq_recv, g_rows, both, keep, d_send, d_recv, r1_send, r1_recv, fin, e_send, e_recv, scale_s,
    loc_sem, g_send, g_near, g_pair, e_sem, t_sem, z_sem, yt_sem, y_sem, f_sem, q_sem, ds_sem, dr_sem, rs_sem, rr_sem,
):
    seq = lax.axis_index("seq")
    tp = lax.axis_index("tp")
    x = tp // 2
    c = tp % 2
    y = seq // 8
    z = seq % 8
    partner = 2 * x + (1 - c)
    rx, lx, ox = (x + 1) % 4, (x + 3) % 4, (x + 2) % 4
    right, left, opp = 2 * rx + c, 2 * lx + c, 2 * ox + c
    nxt, prv = (seq + 1) % 32, (seq + 31) % 32

    def remote(src, dst, ssem, rsem, **where):
        return pltpu.make_async_remote_copy(
            src_ref=src, dst_ref=dst, send_sem=ssem, recv_sem=rsem, device_id=where, device_id_type=MESH
        )

    phase = Phases()
    phase("start")
    copies = (
        (tok, tok_t, 0), (w_inner, wall.at[:, 0:CH], 1), (w_state, wall.at[:, CH:CONV], 1), (w_step, step_t, 2),
        (bias, vec.at[0:1], 3), (rate, vec.at[1:2], 3), (skip, vec.at[2:3], 3), (k_inner, kern.at[:, 0:CH], 4),
        (k_state, kern.at[:, CH:CONV], 4), (gain, gain_v, 5), (w_gate, wg, 6), (w_out, wo, 7),
    )
    for src, dst, i in copies:
        pltpu.make_async_copy(src, dst, loc_sem.at[i]).start()

    def loaded(ref, i):
        pltpu.make_async_copy(ref, ref, loc_sem.at[i]).wait()

    barrier = pltpu.get_barrier_semaphore()
    for k in range(1, 8):
        pl.semaphore_signal(barrier, inc=1, device_id={"tp": (tp + k) % 8}, device_id_type=MESH)
    for k in range(1, 8):
        pl.semaphore_signal(barrier, inc=1, device_id={"seq": y * 8 + (z + k) % 8}, device_id_type=MESH)
    for k in range(1, 4):
        pl.semaphore_signal(barrier, inc=1, device_id={"seq": ((y + k) % 4) * 8 + z}, device_id_type=MESH)
    for s in (nxt, prv):
        pl.semaphore_signal(barrier, inc=1, device_id={"seq": s}, device_id_type=MESH)

    er = lax.broadcasted_iota(jnp.int32, (ST, CH), 0)
    ec = lax.broadcasted_iota(jnp.int32, (ST, CH), 1)
    off = ec - er * 64
    expand[...] = jnp.where((off >= 0) & (off < 64), 1.0, 0.0).astype(BF16)
    small[...] = jnp.zeros_like(small)

    def expanded(v):
        hi, lo = split2(v)
        return dot(hi, expand[...]) + dot(lo, expand[...])

    phase("turn")
    loaded(tok_t, 0)
    xb[tp] = tok_t[...].T
    phase("barrier")
    pl.semaphore_wait(barrier, 19)

    phase("send")
    def piece(src, q, to, sem):
        start, rows = PIECES[q]
        part = xb.at[src, pl.ds(start, rows), :]
        return remote(part, part, g_send.at[0], sem, tp=to)

    def send(src, q, to, origin):
        piece(src, q, to, g_pair.at[origin, int(q in (2, 3, 5))] if to is partner else g_near.at[origin, q]).start()

    def arrived(src, q, origin):
        piece(src, q, partner, g_near.at[origin, q]).wait_recv()

    def pair_arrived(src, rows, origin):
        part = xb.at[src, pl.ds(rows[0], rows[1]), :]
        remote(part, part, g_send.at[0], g_pair.at[origin, 1 if rows[0] else 0], tp=partner).wait_recv()

    for a, b in ((2, 3), (3, 2), (4, 4)):
        send(tp, a, right, 0)
        send(tp, b, left, 1)
    for q in (5, 4):
        send(tp, q, partner, 3)
    phase("step_turn")
    loaded(step_t, 2)
    step_f[...] = jnp.zeros_like(step_f)
    step_f[0:HD, :] = step_t[...].astype(F32)
    wall[:, CONV:WIDE] = step_f[...].T.astype(BF16)
    loaded(vec, 3)
    for i in range(3):
        small[8 * i : 8 * i + 1, 0:HD] = vec[i : i + 1, :]
    loaded(wall.at[:, 0:CONV], 1)

    def accumulate(src, start, rows, first=False):
        rr = pl.ds(start, rows)
        v = dot(xb[src, rr, :], wall[pl.ds(pl.multiple_of(src * KD, 64), KD), :])
        acc[rr, :] = v if first else acc[rr, :] + v

    early, late = (EARLY, ROWS - EARLY), (0, EARLY)
    rp, lp, op = 2 * rx + 1 - c, 2 * lx + 1 - c, 2 * ox + 1 - c
    phase("own")
    accumulate(tp, *early, True)
    accumulate(tp, *late, True)
    pair_arrived(partner, early, 3)
    accumulate(partner, *early)
    pair_arrived(partner, late, 3)
    accumulate(partner, *late)
    phase("near0")
    arrived(left, 2, 0)
    send(left, 2, right, 2)
    send(left, 2, partner, 0)
    arrived(right, 3, 1)
    send(right, 3, left, 2)
    send(right, 3, partner, 1)
    phase("near1")
    arrived(left, 3, 0)
    send(left, 3, partner, 0)
    arrived(right, 2, 1)
    send(right, 2, partner, 1)
    phase("near_early")
    accumulate(left, *early)
    accumulate(right, *early)
    phase("nearp_early")
    pair_arrived(lp, early, 0)
    accumulate(lp, *early)
    pair_arrived(rp, early, 1)
    accumulate(rp, *early)
    phase("near2")
    arrived(left, 4, 0)
    send(left, 0, right, 2)
    send(left, 4, partner, 0)
    arrived(right, 4, 1)
    send(right, 1, left, 2)
    send(right, 4, partner, 1)
    phase("near_late")
    accumulate(left, *late)
    accumulate(right, *late)
    phase("nearp_late")
    pair_arrived(lp, late, 0)
    accumulate(lp, *late)
    pair_arrived(rp, late, 1)
    accumulate(rp, *late)
    phase("far_early")
    for q in (2, 3):
        arrived(opp, q, 2)
        send(opp, q, partner, 2)
    accumulate(opp, *early)
    phase("farp_early")
    pair_arrived(op, early, 2)
    accumulate(op, *early)

    phase("edge")
    edge_s[...] = acc[ROWS - 16 : ROWS, 0:CONV].astype(BF16)
    edge = remote(edge_s, edge_r, e_sem.at[0], e_sem.at[1], seq=nxt)
    edge.start()
    mx[8 + EARLY : 8 + ROWS, :] = acc[EARLY:ROWS, 0:CONV].astype(BF16).astype(F32)

    tri = (
        lax.broadcasted_iota(jnp.int32, (GROUP, GROUP), 0) >= lax.broadcasted_iota(jnp.int32, (GROUP, GROUP), 1)
    ).astype(BF16)

    def steps(b):
        rr = slice(b * GROUP, (b + 1) * GROUP)
        raw = acc[rr, CONV:WIDE] + small[0:1, :]
        dt = jnp.maximum(raw, 0.0) + jnp.log1p(jnp.exp(-jnp.abs(raw)))
        ld = -dt * small[8:9, :]
        hi = ld.astype(BF16)
        mid, low = split2(ld - hi.astype(F32))
        cum = dot(tri, hi) + dot(tri, mid) + dot(tri, low)
        cum_s[rr, :] = cum
        dt_s[rr, :] = dt

    def conv(b, first=0, last=CONV // 128 - 1):
        def body(j, carry):
            cols = pl.ds(pl.multiple_of(j * 128, 128), 128)

            def taps(ref, kcols):
                total = mx[pl.ds(b * GROUP + 5, GROUP), cols] * ref[0:1, kcols]
                for k in range(1, 4):
                    total = total + mx[pl.ds(b * GROUP + 5 + k, GROUP), cols] * ref[k : k + 1, kcols]
                return silu(total).astype(BF16)

            act[pl.ds(b * GROUP, GROUP), cols] = taps(kern, cols)
            return carry

        lax.fori_loop(first, last, body, 0)

    loaded(kern, 4)

    def contribution(b):
        rr = slice(b * GROUP, (b + 1) * GROUP)
        ending = cum_s[(b + 1) * GROUP - 1 : (b + 1) * GROUP, :]
        tail = jnp.exp(ending - cum_s[rr, :]) * dt_s[rr, :]
        scaled = (act[rr, 0:CH].astype(F32) * expanded(tail)).astype(BF16)
        inject_t = act[rr, CH : CH + ST].astype(F32).T.astype(BF16)
        return dot(inject_t, scaled)

    phase("steps1")
    steps(1)
    phase("far_late")
    for q in (0, 1):
        arrived(opp, q, 2)
        send(opp, q, partner, 2)
    phase("conv1")
    conv(1)
    phase("contrib1")
    st_f[...] = contribution(1)
    phase("far_acc")
    accumulate(opp, *late)
    phase("farp_late")
    pair_arrived(op, late, 2)
    accumulate(op, *late)
    mx[8 : 8 + EARLY, :] = acc[0:EARLY, 0:CONV].astype(BF16).astype(F32)
    phase("steps0")
    steps(0)
    ends = jnp.concatenate([cum_s[GROUP - 1 : GROUP, :], cum_s[ROWS - 1 : ROWS, :]], axis=0)
    total = ends[0:1, :] + ends[1:2, :]
    row8 = lax.broadcasted_iota(jnp.int32, (8, ST), 0)
    t_send[...] = jnp.where(row8 == z, total, 0.0)

    for k in (4, 3, 5, 2, 6, 1, 7):
        remote(t_send, t_recv.at[z], t_sem.at[0], t_sem.at[1], seq=y * 8 + (z + k) % 8).start()
    t_recv[z] = t_send[...]

    phase("edge_wait")
    edge.wait_recv()
    halo = edge_r[8:16, :].astype(F32)
    mx[0:8, :] = jnp.where(seq == 0, 0.0, halo)
    phase("conv0")
    conv(0)
    phase("contrib0")
    c0_s[...] = contribution(0)
    ends8 = jnp.concatenate([ends, jnp.zeros((6, ST), F32)], axis=0)
    end_exp = expanded(jnp.exp(ends8))
    st_bf[...] = (end_exp[1:2, :] * c0_s[...] + st_f[...]).astype(BF16)
    phase("zsend")
    for k in (4, 3, 5, 2, 6, 1, 7):
        to = (z + k) % 8
        part = st_bf.at[pl.ds(pl.multiple_of(16 * to, 16), 16), :]
        remote(part, z_recv.at[z], z_sem.at[0], z_sem.at[1], seq=y * 8 + to).start()
    z_recv[z] = st_bf[pl.ds(pl.multiple_of(16 * z, 16), 16), :]

    phase("late_steps")
    for b in range(2):
        conv(b, CONV // 128 - 1, CONV // 128)
    for b in range(2):
        rr = slice(b * GROUP, (b + 1) * GROUP)
        cumt_s[b] = (cum_s[rr, :] * LOG2E).T[0:16, :]
        dtt_s[b] = dt_s[rr, :].T[0:16, :]
        gexp[rr, :] = expanded(jnp.exp(cum_s[rr, :]))

    def intra(b, rr0):
        t0 = pl.ds(rr0, 128)
        t1 = pl.ds(rr0 + 128, 128)
        both = pl.ds(rr0, GROUP)
        inject = act[both, CH : CH + ST]
        sc0 = dot_nt(act[t0, CH + ST : CONV], inject[0:128, :])
        sc1 = dot_nt(act[t1, CH + ST : CONV], inject)
        diag = lax.broadcasted_iota(jnp.int32, (128, 128), 0) >= lax.broadcasted_iota(jnp.int32, (128, 128), 1)
        lane = lax.broadcasted_iota(jnp.int32, (128, 128), 1) < 64
        ca = cum_s[t0, :] * LOG2E
        cb = cum_s[t1, :] * LOG2E
        for p in range(HD // 2):
            cols = slice(p * 128, (p + 1) * 128)
            chan = act[both, cols]
            res0, res1 = [], []
            for h in (2 * p, 2 * p + 1):
                ct = cumt_s[b, h : h + 1, :]
                dtr = dtt_s[b, h : h + 1, :]
                g0 = jnp.where(diag, ca[:, h : h + 1] - ct[:, 0:128], -1e30)
                m0 = (sc0 * jnp.exp2(g0) * dtr[:, 0:128]).astype(BF16)
                res0.append(dot(m0, chan[0:128, :]))
                g1 = cb[:, h : h + 1] - ct[:, 0:128]
                m1 = (sc1[:, 0:128] * jnp.exp2(g1) * dtr[:, 0:128]).astype(BF16)
                g2 = jnp.where(diag, cb[:, h : h + 1] - ct[:, 128:256], -1e30)
                m2 = (sc1[:, 128:256] * jnp.exp2(g2) * dtr[:, 128:256]).astype(BF16)
                res1.append(dot(m1, chan[0:128, :]) + dot(m2, chan[128:256, :]))
            ssd[t0, cols] = jnp.where(lane, res0[0], res0[1])
            ssd[t1, cols] = jnp.where(lane, res1[0], res1[1])

    def intra_body(b, carry):
        intra(b, pl.multiple_of(b * GROUP, GROUP))
        return carry

    phase("intra")
    lax.fori_loop(0, 2, intra_body, 0)

    phase("decays")
    def all_arrived(ref, sem):
        remote(ref, ref, sem.at[0], sem.at[1], seq=prv).wait_recv()

    def all_sent(ref, sem):
        remote(ref, ref, sem, sem, seq=prv).wait_send()

    all_arrived(t_recv.at[0:7], t_sem)
    tall = t_recv[0]
    for k in range(1, 8):
        tall = tall + t_recv[k]
    texp = expanded(jnp.exp(tall))
    tsum = jnp.zeros((1, ST), F32)
    tpre = []
    for k in range(8):
        tpre.append(tsum)
        tsum = tsum + tall[k : k + 1, :]
    pexp = expanded(jnp.exp(jnp.concatenate(tpre, axis=0)))
    yt_send[...] = jnp.where(row8 == y, tsum, 0.0)
    for k in range(1, 4):
        to = ((y + k) % 4) * 8 + z
        remote(yt_send, yt_recv.at[y], yt_sem.at[0], yt_sem.at[1], seq=to).start()
    yt_recv[y] = yt_send[...]

    phase("zwait")
    all_arrived(z_recv.at[0:7], z_sem)
    phase("prefix")
    prefix = jnp.zeros((16, CH), F32)
    for k in range(8):
        pref[16 * k : 16 * (k + 1), 0:CH] = prefix
        prefix = texp[k : k + 1, :] * prefix + z_recv[k].astype(F32)
    y_send[...] = prefix.astype(BF16)
    for k in (2, 1, 3):
        to = ((y + k) % 4) * 8 + z
        remote(y_send, y_recv.at[y], y_sem.at[0], y_sem.at[1], seq=to).start()
    y_recv[y] = y_send[...]

    phase("gate1")
    loaded(wg, 6)

    def gate_half(half):
        rr = slice(half * GROUP, (half + 1) * GROUP)
        v = dot(xb[0, rr, :], wg[0:KD, :])
        for src in range(1, 8):
            v = v + dot(xb[src, rr, :], wg[src * KD : (src + 1) * KD, :])
        acc_g[rr, :] = silu(v.astype(BF16).astype(F32))

    gate_half(1)
    phase("ywait")
    all_arrived(yt_recv.at[0:3], yt_sem)
    yall = yt_recv[0]
    for k in range(1, 4):
        yall = yall + yt_recv[k]
    yexp = expanded(jnp.exp(yall))
    all_arrived(y_recv.at[0:3], y_sem)
    phase("ycomb")
    run = jnp.zeros((16, CH), F32)
    chosen = run
    for k in range(3):
        run = yexp[k : k + 1, :] * run + y_recv[k].astype(F32)
        chosen = jnp.where(y == k + 1, run, chosen)
    for k in range(8):
        f_send[k] = (pref[16 * k : 16 * (k + 1), 0:CH] + pexp[k : k + 1, :] * chosen).astype(BF16)
    mine = pl.ds(pl.multiple_of(16 * z, 16), 16)
    for k in (4, 3, 5, 2, 6, 1, 7):
        to = (z + k) % 8
        remote(f_send.at[to], inc.at[mine, :], f_sem.at[0], f_sem.at[1], seq=y * 8 + to).start()
    inc[mine, :] = f_send[z]

    phase("skip")
    phase("gate0")
    gate_half(0)
    skips = expanded(small[16:24, :])[0:1, :]
    ssd[...] = ssd[...] + skips * act[:, 0:CH].astype(F32)
    loaded(gain_v, 5)
    loaded(wo, 7)
    phase("fwait")

    all_arrived(inc.at[0:112, :], f_sem)
    phase("gated")
    carr[0] = inc[...]
    carr[1] = (c0_s[...] + end_exp[0:1, :] * inc[...].astype(F32)).astype(BF16)

    ones = jnp.ones((8, CH), BF16)
    gain_row = gain_v[...].reshape(1, CH)

    def gate(j, chip):
        rr = pl.ds(pl.multiple_of(chip * 128, 128), 128)
        reads = dot(act[rr, CH + ST : CONV], carr[chip // 2])
        g = (ssd[rr, :] + reads * gexp[rr, :]) * acc_g[rr, :]
        hi, lo = split2(g * g)
        sq_send[chip] = dot_nt(ones, hi) + dot_nt(ones, lo)
        g_rows[j] = (g * gain_row).astype(BF16)

    def d_slot(j, q):
        return q if j == 0 else 8 if j == 3 else 2 + 2 * j + q % 2

    def part(ref, *at):
        return ref.at[at + (slice(None), pl.ds(0, CUTS[at[-1]][1]))]

    def dcopy(j, q):
        return remote(part(d_send, j, q), part(d_recv, j, q), ds_sem.at[0], dr_sem.at[d_slot(j, q)], tp=partner)

    def project(j, which=range(NQ)):
        for q in which:
            start, width = CUTS[q]
            cols = pl.ds(0, width)
            v = dot(g_rows[j], wo[:, start : start + width])
            both[0, :, cols] = v[0:64, :]
            both[1, :, cols] = v[64:128, :]
            d_send[j, q, :, cols] = both[1 - c, :, cols].astype(BF16)
            dcopy(j, q).start()
            keep[j, q, :, cols] = both[c, :, cols]

    def paired(j, q):
        if j == 0:
            dcopy(j, q).wait_recv()
        elif q < 2 and (j < 3 or q == 0):
            ref = wo.at[0:64, 0 : D if j == 3 else D // 2]
            remote(ref, ref, ds_sem.at[0], dr_sem.at[d_slot(j, q)], tp=partner).wait_recv()
        cols = pl.ds(0, CUTS[q][1])
        return keep[j, q, :, cols] + d_recv[j, q, :, cols].astype(F32)

    def hop1(q):
        to = right if q % 2 == 0 else left
        return remote(part(r1_send, 0, q), part(r1_recv, q), rs_sem.at[0], rr_sem.at[q], tp=to)

    def direct(way):
        to = left if way == 0 else right
        return remote(e_send.at[way], e_recv.at[way], rs_sem.at[0], rr_sem.at[NQ + way], tp=to)

    def hop2(q):
        to = right if q % 2 == 0 else left
        return remote(part(r1_send, 1, q), part(fin, q), rs_sem.at[0], rr_sem.at[NQ + 2 + q], tp=to)

    def within(q):
        start, width = CUTS[q]
        return pl.ds(start % (D // 2), width)

    def put(which, q, value):
        r1_send[which, q, :, pl.ds(0, CUTS[q][1])] = value.astype(BF16)

    def hop1_start(q):
        put(0, q, paired(0, q))
        hop1(q).start()

    gate(0, ox)
    project(0)
    phase("hop1")
    hop1_start(0)
    hop1_start(1)
    phase("block1")
    gate(1, lx)
    phase("hop1b")
    hop1_start(2)
    hop1_start(3)
    phase("block12")
    project(1, (0, 2))
    gate(2, rx)
    project(2, (1, 3))
    gate(3, x)
    for k in range(1, 8):
        to = (tp + k) % 8
        remote(sq_send.at[to // 2], sq_recv.at[tp], q_sem.at[0], q_sem.at[1], tp=to).start()
    sq_recv[tp] = sq_send[x]
    phase("block12b")
    project(1, (1, 3))
    phase("direct")
    for q in (0, 2, 1, 3):
        e_send[q % 2, :, within(q)] = paired(1 if q % 2 == 0 else 2, q).astype(BF16)
        if q >= 2:
            direct(q % 2).start()
    phase("block23")
    project(2, (0, 2))
    project(3)
    phase("hop2")
    for q in range(NQ):
        v = paired(2 if q % 2 == 0 else 1, q)
        hop1(q).wait_recv()
        put(1, q, v + r1_recv[q, :, pl.ds(0, CUTS[q][1])].astype(F32))
        hop2(q).start()
    phase("own_sum")
    for q in range(NQ):
        keep[3, q, :, pl.ds(0, CUTS[q][1])] = paired(3, q)
    phase("scale")
    tiles = sq_recv.at[0:7]
    remote(tiles, tiles, q_sem.at[0], q_sem.at[1], tp=partner).wait_recv()
    sq = sq_recv[0]
    for k in range(1, 8):
        sq = sq + sq_recv[k]
    factor = lax.rsqrt(sq * (1.0 / INNER) + 1e-5)
    scale_s[...] = jnp.broadcast_to(factor[0:1, :], (128, 128)).T
    scale = scale_s[pl.ds(pl.multiple_of(64 * c, 64), 64), :]
    for q, (start, width) in enumerate(CUTS):
        if q < 2:
            direct(q).wait_recv()
        hop2(q).wait_recv()
        shift = start % (D // 2)
        for j in range(width // 128):
            cols = slice(j * 128, (j + 1) * 128)
            more = slice(shift + j * 128, shift + (j + 1) * 128)
            v = keep[3, q, :, cols] + fin[q, :, cols].astype(F32) + e_recv[q % 2, :, more].astype(F32)
            out[:, start + j * 128 : start + (j + 1) * 128] = (v * scale).astype(BF16)
    phase("drain")
    edge.wait_send()
    for ref, sem in (
        (xb.at[0:7], g_send), (t_recv.at[0:7], t_sem), (z_recv.at[0:7], z_sem), (yt_recv.at[0:3], yt_sem),
        (y_recv.at[0:3], y_sem), (f_send.at[0:7], f_sem), (sq_recv.at[0:7], q_sem),
        (wo.at[0:256, :], ds_sem), (wo.at[0:192, :], rs_sem),
    ):
        all_sent(ref, sem.at[0])
    phase.close()


def on_device(tok, w_gate, w_inner, w_state, w_step, k_inner, k_state, bias, rate, skip, gain, w_out):
    vm = pltpu.VMEM
    dma = pltpu.SemaphoreType.DMA
    scratch = [
        vm((8, ROWS, KD), BF16), vm((KD, ROWS), BF16), vm((HD, D), BF16), vm((ST, D), F32), vm((D, CH), BF16), vm((D, WIDE), BF16),
        vm((CH, D), BF16), vm((4, CONV), F32), vm((3, HD), F32), vm((CH,), F32),
        vm((ROWS, WIDE), F32), vm((ROWS, CH), F32),
        vm((8 + ROWS, CONV), F32), vm((ROWS, CONV), BF16), vm((16, CONV), BF16), vm((16, CONV), BF16),
        vm((24, ST), F32), vm((ST, CH), BF16), vm((ROWS, ST), F32), vm((ROWS, ST), F32),
        vm((2, 16, GROUP), F32), vm((2, 16, GROUP), F32),
        vm((ROWS, CH), F32), vm((ROWS, CH), F32), vm((ST, CH), BF16), vm((ST, CH), F32), vm((ST, CH), F32),
        vm((8, 16, CH), BF16), vm((8, ST), F32), vm((8, 8, ST), F32), vm((ST, CONV), F32),
        vm((16, CH), BF16), vm((8, ST), F32), vm((4, 16, CH), BF16), vm((4, 8, ST), F32),
        vm((8, 16, CH), BF16), vm((ST, CH), BF16), vm((2, ST, CH), BF16),
        vm((4, 8, ST), F32), vm((8, 8, ST), F32), vm((4, ST, CH), BF16), vm((2, 64, QC), F32),
        vm((4, NQ, 64, QC), F32), vm((4, NQ, 64, QC), BF16), vm((4, NQ, 64, QC), BF16),
        vm((2, NQ, 64, QC), BF16), vm((NQ, 64, QC), BF16), vm((NQ, 64, QC), BF16),
        vm((2, 64, D // 2), BF16), vm((2, 64, D // 2), BF16), vm((128, 128), F32),
        dma((8,)), dma((1,)), dma((3, 5)), dma((4, 2)), dma((2,)), dma((2,)), dma((2,)), dma((2,)), dma((2,)), dma((2,)),
        dma((2,)), dma((1,)), dma((9,)), dma((1,)), dma((2 * NQ + 2,)),
    ]
    hbm = pl.BlockSpec(memory_space=pl.ANY)
    local = pl.BlockSpec(memory_space=pltpu.VMEM)
    return pl.pallas_call(
        kernel,
        name="layer",
        out_shape=pltpu.VMEM((ROWS // 8, D), BF16),
        in_specs=[hbm] * 12,
        out_specs=local,
        scratch_shapes=scratch,
        compiler_params=pltpu.CompilerParams(
            collective_id=0, has_side_effects=True, vmem_limit_bytes=62 * 1024 * 1024
        ),
    )(
        tok.T, w_gate, w_inner, w_state, w_step.T, k_inner, k_state,
        bias.reshape(1, -1), rate.reshape(1, -1), skip.reshape(1, -1), gain, w_out,
    )


def solution(mesh):
    return jax.shard_map(
        on_device,
        mesh=mesh,
        in_specs=(
            P("seq", "tp"), P(None, "tp"), P(None, "tp"), P(), P(None, "tp"), P(None, "tp"), P(),
            P("tp"), P("tp"), P("tp"), P("tp"), P("tp", None),
        ),
        out_specs=P(("seq", "tp"), None),
        check_vma=False,
    )
```

```python
import jax
import jax.numpy as jnp
from jax import lax
from jax.experimental import pallas as pl
from jax.experimental.pallas import tpu as pltpu
from jax.sharding import PartitionSpec as P

MESH = pl.DeviceIdType.MESH
F32 = jnp.float32
BF16 = jnp.bfloat16
ROWS = 512
GROUP = 256
KD = 320
D = 2560
CH = 640
HD = 10
ST = 128
CONV = CH + 2 * ST
WIDE = CONV + ST
CUTS = ((0, 512), (1280, 512), (512, 768), (1792, 768))
NQ = len(CUTS)
PIECES = ((0, 112), (112, 128), (240, 144), (384, 128), (0, 240), (240, 272))
EARLY = 240
QC = 768
LOG2E = 1.4426950408889634
INNER = 5120


def split2(v):
    hi = v.astype(BF16)
    return hi, (v - hi.astype(F32)).astype(BF16)


def dot(a, b):
    return jnp.dot(a, b, preferred_element_type=F32)


def dot_nt(a, b):
    return lax.dot_general(a, b, (((1,), (1,)), ((), ())), preferred_element_type=F32)


class Phases:
    open_scope = None

    def __call__(self, name):
        self.close()
        self.open_scope = jax.named_scope(name)
        self.open_scope.__enter__()

    def close(self):
        if self.open_scope is not None:
            self.open_scope.__exit__(None, None, None)
            self.open_scope = None


def silu(v):
    return 0.5 * v * (1.0 + jnp.tanh(0.5 * v))


def kernel(
    tok, w_gate, w_inner, w_state, w_step, k_inner, k_state, bias, rate, skip, gain, w_out,
    out,
    xb, tok_t, step_t, step_f, wg, wall, wo, kern, vec, gain_v,
    acc, acc_g, mx, act, edge_s, edge_r,
    small, expand, cum_s, dt_s, cumt_s, dtt_s,
    ssd, gexp, st_bf, st_f, c0_s, z_recv, t_send, t_recv, pref, y_send, yt_send, y_recv, yt_recv, f_send, inc, carr,
    sq_send, sq_recv, g_rows, both, keep, d_send, d_recv, r1_send, r1_recv, fin, e_send, e_recv, scale_s,
    loc_sem, g_send, g_near, g_pair, e_sem, t_sem, z_sem, yt_sem, y_sem, f_sem, q_sem, ds_sem, dr_sem, rs_sem, rr_sem,
):
    seq = lax.axis_index("seq")
    tp = lax.axis_index("tp")
    x = tp // 2
    c = tp % 2
    y = seq // 8
    z = seq % 8
    partner = 2 * x + (1 - c)
    rx, lx, ox = (x + 1) % 4, (x + 3) % 4, (x + 2) % 4
    right, left, opp = 2 * rx + c, 2 * lx + c, 2 * ox + c
    nxt, prv = (seq + 1) % 32, (seq + 31) % 32

    def remote(src, dst, ssem, rsem, **where):
        return pltpu.make_async_remote_copy(
            src_ref=src, dst_ref=dst, send_sem=ssem, recv_sem=rsem, device_id=where, device_id_type=MESH
        )

    phase = Phases()
    phase("start")
    barrier = pltpu.get_barrier_semaphore()
    for k in range(1, 8):
        pl.semaphore_signal(barrier, inc=1, device_id={"tp": (tp + k) % 8}, device_id_type=MESH)
    for k in range(1, 8):
        pl.semaphore_signal(barrier, inc=1, device_id={"seq": y * 8 + (z + k) % 8}, device_id_type=MESH)
    for k in range(1, 4):
        pl.semaphore_signal(barrier, inc=1, device_id={"seq": ((y + k) % 4) * 8 + z}, device_id_type=MESH)
    for s in (nxt, prv):
        pl.semaphore_signal(barrier, inc=1, device_id={"seq": s}, device_id_type=MESH)

    copies = (
        (tok, tok_t, 0), (w_inner, wall.at[:, 0:CH], 1), (w_state, wall.at[:, CH:CONV], 1), (w_step, step_t, 2),
        (bias, vec.at[0:1], 3), (rate, vec.at[1:2], 3), (skip, vec.at[2:3], 3), (k_inner, kern.at[:, 0:CH], 4),
        (k_state, kern.at[:, CH:CONV], 4), (gain, gain_v, 5), (w_gate, wg, 6), (w_out, wo, 7),
    )
    for src, dst, i in copies:
        pltpu.make_async_copy(src, dst, loc_sem.at[i]).start()

    def loaded(ref, i):
        pltpu.make_async_copy(ref, ref, loc_sem.at[i]).wait()

    def expanded(v):
        hi, lo = split2(v)
        return dot(hi, expand[...]) + dot(lo, expand[...])

    phase("turn")
    loaded(tok_t, 0)
    xb[tp] = tok_t[...].T
    phase("barrier")
    pl.semaphore_wait(barrier, 19)

    phase("send")
    def piece(src, q, to, sem):
        start, rows = PIECES[q]
        part = xb.at[src, pl.ds(start, rows), :]
        return remote(part, part, g_send.at[0], sem, tp=to)

    def send(src, q, to, origin):
        piece(src, q, to, g_pair.at[origin, int(q in (2, 3, 5))] if to is partner else g_near.at[origin, q]).start()

    def arrived(src, q, origin):
        piece(src, q, partner, g_near.at[origin, q]).wait_recv()

    def pair_arrived(src, rows, origin):
        part = xb.at[src, pl.ds(rows[0], rows[1]), :]
        remote(part, part, g_send.at[0], g_pair.at[origin, 1 if rows[0] else 0], tp=partner).wait_recv()

    for q in (5, 4):
        send(tp, q, right, 0)
        send(tp, q, left, 1)
    for q in (5, 4):
        send(tp, q, partner, 3)
    phase("step_turn")
    er = lax.broadcasted_iota(jnp.int32, (ST, CH), 0)
    ec = lax.broadcasted_iota(jnp.int32, (ST, CH), 1)
    off = ec - er * 64
    expand[...] = jnp.where((off >= 0) & (off < 64), 1.0, 0.0).astype(BF16)
    small[...] = jnp.zeros_like(small)
    loaded(step_t, 2)
    step_f[...] = jnp.zeros_like(step_f)
    step_f[0:HD, :] = step_t[...].astype(F32)
    wall[:, CONV:WIDE] = step_f[...].T.astype(BF16)
    loaded(vec, 3)
    for i in range(3):
        small[8 * i : 8 * i + 1, 0:HD] = vec[i : i + 1, :]
    loaded(wall.at[:, 0:CONV], 1)

    def accumulate(src, start, rows, first=False):
        rr = pl.ds(start, rows)
        v = dot(xb[src, rr, :], wall[pl.ds(pl.multiple_of(src * KD, 64), KD), :])
        acc[rr, :] = v if first else acc[rr, :] + v

    early, late = (EARLY, ROWS - EARLY), (0, EARLY)
    rp, lp, op = 2 * rx + 1 - c, 2 * lx + 1 - c, 2 * ox + 1 - c
    phase("own")
    accumulate(tp, *early, True)
    accumulate(tp, *late, True)
    pair_arrived(partner, early, 3)
    accumulate(partner, *early)
    pair_arrived(partner, late, 3)
    accumulate(partner, *late)
    phase("near0")
    arrived(left, 5, 0)
    send(left, 2, right, 2)
    send(left, 5, partner, 0)
    arrived(right, 5, 1)
    send(right, 3, left, 2)
    send(right, 5, partner, 1)
    phase("near_early")
    accumulate(left, *early)
    accumulate(right, *early)
    phase("nearp_early")
    pair_arrived(lp, early, 0)
    accumulate(lp, *early)
    pair_arrived(rp, early, 1)
    accumulate(rp, *early)
    phase("near2")
    arrived(left, 4, 0)
    send(left, 0, right, 2)
    send(left, 4, partner, 0)
    arrived(right, 4, 1)
    send(right, 1, left, 2)
    send(right, 4, partner, 1)
    phase("near_late")
    accumulate(left, *late)
    accumulate(right, *late)
    phase("nearp_late")
    pair_arrived(lp, late, 0)
    accumulate(lp, *late)
    pair_arrived(rp, late, 1)
    accumulate(rp, *late)
    phase("far_early")
    for q in (2, 3):
        arrived(opp, q, 2)
        send(opp, q, partner, 2)
    accumulate(opp, *early)
    phase("farp_early")
    pair_arrived(op, early, 2)
    accumulate(op, *early)

    phase("edge")
    edge_s[...] = acc[ROWS - 16 : ROWS, 0:CONV].astype(BF16)
    edge = remote(edge_s, edge_r, e_sem.at[0], e_sem.at[1], seq=nxt)
    edge.start()
    mx[8 + EARLY : 8 + ROWS, :] = acc[EARLY:ROWS, 0:CONV].astype(BF16).astype(F32)

    tri = (
        lax.broadcasted_iota(jnp.int32, (GROUP, GROUP), 0) >= lax.broadcasted_iota(jnp.int32, (GROUP, GROUP), 1)
    ).astype(BF16)

    def steps(b):
        rr = slice(b * GROUP, (b + 1) * GROUP)
        raw = acc[rr, CONV:WIDE] + small[0:1, :]
        dt = jnp.maximum(raw, 0.0) + jnp.log1p(jnp.exp(-jnp.abs(raw)))
        ld = -dt * small[8:9, :]
        hi = ld.astype(BF16)
        mid, low = split2(ld - hi.astype(F32))
        cum = dot(tri, hi) + dot(tri, mid) + dot(tri, low)
        cum_s[rr, :] = cum
        dt_s[rr, :] = dt

    def conv(b, first=0, last=CONV // 128 - 1):
        def body(j, carry):
            cols = pl.ds(pl.multiple_of(j * 128, 128), 128)

            def taps(ref, kcols):
                total = mx[pl.ds(b * GROUP + 5, GROUP), cols] * ref[0:1, kcols]
                for k in range(1, 4):
                    total = total + mx[pl.ds(b * GROUP + 5 + k, GROUP), cols] * ref[k : k + 1, kcols]
                return silu(total).astype(BF16)

            act[pl.ds(b * GROUP, GROUP), cols] = taps(kern, cols)
            return carry

        lax.fori_loop(first, last, body, 0)

    loaded(kern, 4)

    def contribution(b):
        rr = slice(b * GROUP, (b + 1) * GROUP)
        ending = cum_s[(b + 1) * GROUP - 1 : (b + 1) * GROUP, :]
        tail = jnp.exp(ending - cum_s[rr, :]) * dt_s[rr, :]
        scaled = (act[rr, 0:CH].astype(F32) * expanded(tail)).astype(BF16)
        inject_t = act[rr, CH : CH + ST].astype(F32).T.astype(BF16)
        return dot(inject_t, scaled)

    phase("steps1")
    steps(1)
    phase("far_late")
    for q in (0, 1):
        arrived(opp, q, 2)
        send(opp, q, partner, 2)
    phase("conv1")
    conv(1)
    phase("contrib1")
    st_f[...] = contribution(1)
    phase("far_acc")
    accumulate(opp, *late)
    phase("farp_late")
    pair_arrived(op, late, 2)
    accumulate(op, *late)
    mx[8 : 8 + EARLY, :] = acc[0:EARLY, 0:CONV].astype(BF16).astype(F32)
    phase("steps0")
    steps(0)
    ends = jnp.concatenate([cum_s[GROUP - 1 : GROUP, :], cum_s[ROWS - 1 : ROWS, :]], axis=0)
    total = ends[0:1, :] + ends[1:2, :]
    row8 = lax.broadcasted_iota(jnp.int32, (8, ST), 0)
    t_send[...] = jnp.where(row8 == z, total, 0.0)

    for k in (4, 3, 5, 2, 6, 1, 7):
        remote(t_send, t_recv.at[z], t_sem.at[0], t_sem.at[1], seq=y * 8 + (z + k) % 8).start()
    t_recv[z] = t_send[...]

    phase("edge_wait")
    edge.wait_recv()
    halo = edge_r[8:16, :].astype(F32)
    mx[0:8, :] = jnp.where(seq == 0, 0.0, halo)
    phase("conv0")
    conv(0)
    phase("contrib0")
    c0_s[...] = contribution(0)
    ends8 = jnp.concatenate([ends, jnp.zeros((6, ST), F32)], axis=0)
    end_exp = expanded(jnp.exp(ends8))
    st_bf[...] = (end_exp[1:2, :] * c0_s[...] + st_f[...]).astype(BF16)
    phase("zsend")
    for k in (4, 3, 5, 2, 6, 1, 7):
        to = (z + k) % 8
        part = st_bf.at[pl.ds(pl.multiple_of(16 * to, 16), 16), :]
        remote(part, z_recv.at[z], z_sem.at[0], z_sem.at[1], seq=y * 8 + to).start()
    z_recv[z] = st_bf[pl.ds(pl.multiple_of(16 * z, 16), 16), :]

    phase("late_steps")
    for b in range(2):
        conv(b, CONV // 128 - 1, CONV // 128)
    for b in range(2):
        rr = slice(b * GROUP, (b + 1) * GROUP)
        cumt_s[b] = (cum_s[rr, :] * LOG2E).T[0:16, :]
        dtt_s[b] = dt_s[rr, :].T[0:16, :]
        gexp[rr, :] = expanded(jnp.exp(cum_s[rr, :]))

    def intra(b, rr0):
        t0 = pl.ds(rr0, 128)
        t1 = pl.ds(rr0 + 128, 128)
        both = pl.ds(rr0, GROUP)
        inject = act[both, CH : CH + ST]
        sc0 = dot_nt(act[t0, CH + ST : CONV], inject[0:128, :])
        sc1 = dot_nt(act[t1, CH + ST : CONV], inject)
        diag = lax.broadcasted_iota(jnp.int32, (128, 128), 0) >= lax.broadcasted_iota(jnp.int32, (128, 128), 1)
        lane = lax.broadcasted_iota(jnp.int32, (128, 128), 1) < 64
        ca = cum_s[t0, :] * LOG2E
        cb = cum_s[t1, :] * LOG2E
        for p in range(HD // 2):
            cols = slice(p * 128, (p + 1) * 128)
            chan = act[both, cols]
            res0, res1 = [], []
            for h in (2 * p, 2 * p + 1):
                ct = cumt_s[b, h : h + 1, :]
                dtr = dtt_s[b, h : h + 1, :]
                g0 = jnp.where(diag, ca[:, h : h + 1] - ct[:, 0:128], -1e30)
                m0 = (sc0 * jnp.exp2(g0) * dtr[:, 0:128]).astype(BF16)
                res0.append(dot(m0, chan[0:128, :]))
                g1 = cb[:, h : h + 1] - ct[:, 0:128]
                m1 = (sc1[:, 0:128] * jnp.exp2(g1) * dtr[:, 0:128]).astype(BF16)
                g2 = jnp.where(diag, cb[:, h : h + 1] - ct[:, 128:256], -1e30)
                m2 = (sc1[:, 128:256] * jnp.exp2(g2) * dtr[:, 128:256]).astype(BF16)
                res1.append(dot(m1, chan[0:128, :]) + dot(m2, chan[128:256, :]))
            ssd[t0, cols] = jnp.where(lane, res0[0], res0[1])
            ssd[t1, cols] = jnp.where(lane, res1[0], res1[1])

    def intra_body(b, carry):
        intra(b, pl.multiple_of(b * GROUP, GROUP))
        return carry

    phase("intra")
    lax.fori_loop(0, 2, intra_body, 0)

    phase("decays")
    def all_arrived(ref, sem):
        remote(ref, ref, sem.at[0], sem.at[1], seq=prv).wait_recv()

    def all_sent(ref, sem):
        remote(ref, ref, sem, sem, seq=prv).wait_send()

    all_arrived(t_recv.at[0:7], t_sem)
    tall = t_recv[0]
    for k in range(1, 8):
        tall = tall + t_recv[k]
    texp = expanded(jnp.exp(tall))
    tsum = jnp.zeros((1, ST), F32)
    tpre = []
    for k in range(8):
        tpre.append(tsum)
        tsum = tsum + tall[k : k + 1, :]
    pexp = expanded(jnp.exp(jnp.concatenate(tpre, axis=0)))
    yt_send[...] = jnp.where(row8 == y, tsum, 0.0)
    for k in range(1, 4):
        to = ((y + k) % 4) * 8 + z
        remote(yt_send, yt_recv.at[y], yt_sem.at[0], yt_sem.at[1], seq=to).start()
    yt_recv[y] = yt_send[...]

    phase("zwait")
    all_arrived(z_recv.at[0:7], z_sem)
    phase("prefix")
    prefix = jnp.zeros((16, CH), F32)
    for k in range(8):
        pref[16 * k : 16 * (k + 1), 0:CH] = prefix
        prefix = texp[k : k + 1, :] * prefix + z_recv[k].astype(F32)
    y_send[...] = prefix.astype(BF16)
    for k in (2, 1, 3):
        to = ((y + k) % 4) * 8 + z
        remote(y_send, y_recv.at[y], y_sem.at[0], y_sem.at[1], seq=to).start()
    y_recv[y] = y_send[...]

    phase("gate1")
    loaded(wg, 6)

    def gate_half(half):
        rr = slice(half * GROUP, (half + 1) * GROUP)
        v = dot(xb[0, rr, :], wg[0:KD, :])
        for src in range(1, 8):
            v = v + dot(xb[src, rr, :], wg[src * KD : (src + 1) * KD, :])
        acc_g[rr, :] = silu(v.astype(BF16).astype(F32))

    gate_half(1)
    phase("ywait")
    all_arrived(yt_recv.at[0:3], yt_sem)
    yall = yt_recv[0]
    for k in range(1, 4):
        yall = yall + yt_recv[k]
    yexp = expanded(jnp.exp(yall))
    all_arrived(y_recv.at[0:3], y_sem)
    phase("ycomb")
    run = jnp.zeros((16, CH), F32)
    chosen = run
    for k in range(3):
        run = yexp[k : k + 1, :] * run + y_recv[k].astype(F32)
        chosen = jnp.where(y == k + 1, run, chosen)
    for k in range(8):
        f_send[k] = (pref[16 * k : 16 * (k + 1), 0:CH] + pexp[k : k + 1, :] * chosen).astype(BF16)
    mine = pl.ds(pl.multiple_of(16 * z, 16), 16)
    for k in (4, 3, 5, 2, 6, 1, 7):
        to = (z + k) % 8
        remote(f_send.at[to], inc.at[mine, :], f_sem.at[0], f_sem.at[1], seq=y * 8 + to).start()
    inc[mine, :] = f_send[z]

    phase("skip")
    phase("gate0")
    gate_half(0)
    skips = expanded(small[16:24, :])[0:1, :]
    ssd[...] = ssd[...] + skips * act[:, 0:CH].astype(F32)
    loaded(gain_v, 5)
    loaded(wo, 7)
    phase("fwait")

    all_arrived(inc.at[0:112, :], f_sem)
    phase("gated")
    carr[0] = inc[...]
    carr[1] = (c0_s[...] + end_exp[0:1, :] * inc[...].astype(F32)).astype(BF16)

    ones = jnp.ones((8, CH), BF16)
    gain_row = gain_v[...].reshape(1, CH)

    def gate(j, chip):
        rr = pl.ds(pl.multiple_of(chip * 128, 128), 128)
        reads = dot(act[rr, CH + ST : CONV], carr[chip // 2])
        g = (ssd[rr, :] + reads * gexp[rr, :]) * acc_g[rr, :]
        hi, lo = split2(g * g)
        sq_send[chip] = dot_nt(ones, hi) + dot_nt(ones, lo)
        g_rows[j] = (g * gain_row).astype(BF16)

    def d_slot(j, q):
        return q if j == 0 else 8 if j == 3 else 2 + 2 * j + q % 2

    def part(ref, *at):
        return ref.at[at + (slice(None), pl.ds(0, CUTS[at[-1]][1]))]

    def dcopy(j, q):
        return remote(part(d_send, j, q), part(d_recv, j, q), ds_sem.at[0], dr_sem.at[d_slot(j, q)], tp=partner)

    def project(j, which=range(NQ)):
        for q in which:
            start, width = CUTS[q]
            cols = pl.ds(0, width)
            v = dot(g_rows[j], wo[:, start : start + width])
            both[0, :, cols] = v[0:64, :]
            both[1, :, cols] = v[64:128, :]
            d_send[j, q, :, cols] = both[1 - c, :, cols].astype(BF16)
            dcopy(j, q).start()
            keep[j, q, :, cols] = both[c, :, cols]

    def paired(j, q):
        if j == 0:
            dcopy(j, q).wait_recv()
        elif q < 2 and (j < 3 or q == 0):
            ref = wo.at[0:64, 0 : D if j == 3 else D // 2]
            remote(ref, ref, ds_sem.at[0], dr_sem.at[d_slot(j, q)], tp=partner).wait_recv()
        cols = pl.ds(0, CUTS[q][1])
        return keep[j, q, :, cols] + d_recv[j, q, :, cols].astype(F32)

    def hop1(q):
        to = right if q % 2 == 0 else left
        return remote(part(r1_send, 0, q), part(r1_recv, q), rs_sem.at[0], rr_sem.at[q], tp=to)

    def direct(way):
        to = left if way == 0 else right
        return remote(e_send.at[way], e_recv.at[way], rs_sem.at[0], rr_sem.at[NQ + way], tp=to)

    def hop2(q):
        to = right if q % 2 == 0 else left
        return remote(part(r1_send, 1, q), part(fin, q), rs_sem.at[0], rr_sem.at[NQ + 2 + q], tp=to)

    def within(q):
        start, width = CUTS[q]
        return pl.ds(start % (D // 2), width)

    def put(which, q, value):
        r1_send[which, q, :, pl.ds(0, CUTS[q][1])] = value.astype(BF16)

    def hop1_start(q):
        put(0, q, paired(0, q))
        hop1(q).start()

    gate(0, ox)
    project(0)
    phase("hop1")
    hop1_start(0)
    hop1_start(1)
    phase("block1")
    gate(1, lx)
    phase("hop1b")
    hop1_start(2)
    hop1_start(3)
    phase("block12")
    project(1, (0, 2))
    gate(2, rx)
    project(2, (1, 3))
    gate(3, x)
    for k in range(1, 8):
        to = (tp + k) % 8
        remote(sq_send.at[to // 2], sq_recv.at[tp], q_sem.at[0], q_sem.at[1], tp=to).start()
    sq_recv[tp] = sq_send[x]
    phase("block12b")
    project(1, (1, 3))
    phase("direct")
    for q in (0, 2, 1, 3):
        e_send[q % 2, :, within(q)] = paired(1 if q % 2 == 0 else 2, q).astype(BF16)
        if q >= 2:
            direct(q % 2).start()
    phase("block23")
    project(2, (0, 2))
    project(3)
    phase("hop2")
    for q in range(NQ):
        v = paired(2 if q % 2 == 0 else 1, q)
        hop1(q).wait_recv()
        put(1, q, v + r1_recv[q, :, pl.ds(0, CUTS[q][1])].astype(F32))
        hop2(q).start()
    phase("own_sum")
    for q in range(NQ):
        keep[3, q, :, pl.ds(0, CUTS[q][1])] = paired(3, q)
    phase("scale")
    tiles = sq_recv.at[0:7]
    remote(tiles, tiles, q_sem.at[0], q_sem.at[1], tp=partner).wait_recv()
    sq = sq_recv[0]
    for k in range(1, 8):
        sq = sq + sq_recv[k]
    factor = lax.rsqrt(sq * (1.0 / INNER) + 1e-5)
    scale_s[...] = jnp.broadcast_to(factor[0:1, :], (128, 128)).T
    scale = scale_s[pl.ds(pl.multiple_of(64 * c, 64), 64), :]
    for q, (start, width) in enumerate(CUTS):
        if q < 2:
            direct(q).wait_recv()
        hop2(q).wait_recv()
        shift = start % (D // 2)
        for j in range(width // 128):
            cols = slice(j * 128, (j + 1) * 128)
            more = slice(shift + j * 128, shift + (j + 1) * 128)
            v = keep[3, q, :, cols] + fin[q, :, cols].astype(F32) + e_recv[q % 2, :, more].astype(F32)
            out[:, start + j * 128 : start + (j + 1) * 128] = (v * scale).astype(BF16)
    phase("drain")
    edge.wait_send()
    for ref, sem in (
        (xb.at[0:7], g_send), (t_recv.at[0:7], t_sem), (z_recv.at[0:7], z_sem), (yt_recv.at[0:3], yt_sem),
        (y_recv.at[0:3], y_sem), (f_send.at[0:7], f_sem), (sq_recv.at[0:7], q_sem),
        (wo.at[0:256, :], ds_sem), (wo.at[0:192, :], rs_sem),
    ):
        all_sent(ref, sem.at[0])
    phase.close()


def on_device(tok, w_gate, w_inner, w_state, w_step, k_inner, k_state, bias, rate, skip, gain, w_out):
    vm = pltpu.VMEM
    dma = pltpu.SemaphoreType.DMA
    scratch = [
        vm((8, ROWS, KD), BF16), vm((KD, ROWS), BF16), vm((HD, D), BF16), vm((ST, D), F32), vm((D, CH), BF16), vm((D, WIDE), BF16),
        vm((CH, D), BF16), vm((4, CONV), F32), vm((3, HD), F32), vm((CH,), F32),
        vm((ROWS, WIDE), F32), vm((ROWS, CH), F32),
        vm((8 + ROWS, CONV), F32), vm((ROWS, CONV), BF16), vm((16, CONV), BF16), vm((16, CONV), BF16),
        vm((24, ST), F32), vm((ST, CH), BF16), vm((ROWS, ST), F32), vm((ROWS, ST), F32),
        vm((2, 16, GROUP), F32), vm((2, 16, GROUP), F32),
        vm((ROWS, CH), F32), vm((ROWS, CH), F32), vm((ST, CH), BF16), vm((ST, CH), F32), vm((ST, CH), F32),
        vm((8, 16, CH), BF16), vm((8, ST), F32), vm((8, 8, ST), F32), vm((ST, CONV), F32),
        vm((16, CH), BF16), vm((8, ST), F32), vm((4, 16, CH), BF16), vm((4, 8, ST), F32),
        vm((8, 16, CH), BF16), vm((ST, CH), BF16), vm((2, ST, CH), BF16),
        vm((4, 8, ST), F32), vm((8, 8, ST), F32), vm((4, ST, CH), BF16), vm((2, 64, QC), F32),
        vm((4, NQ, 64, QC), F32), vm((4, NQ, 64, QC), BF16), vm((4, NQ, 64, QC), BF16),
        vm((2, NQ, 64, QC), BF16), vm((NQ, 64, QC), BF16), vm((NQ, 64, QC), BF16),
        vm((2, 64, D // 2), BF16), vm((2, 64, D // 2), BF16), vm((128, 128), F32),
        dma((8,)), dma((1,)), dma((3, 6)), dma((4, 2)), dma((2,)), dma((2,)), dma((2,)), dma((2,)), dma((2,)), dma((2,)),
        dma((2,)), dma((1,)), dma((9,)), dma((1,)), dma((2 * NQ + 2,)),
    ]
    hbm = pl.BlockSpec(memory_space=pl.ANY)
    local = pl.BlockSpec(memory_space=pltpu.VMEM)
    return pl.pallas_call(
        kernel,
        name="layer",
        out_shape=pltpu.VMEM((ROWS // 8, D), BF16),
        in_specs=[hbm] * 12,
        out_specs=local,
        scratch_shapes=scratch,
        compiler_params=pltpu.CompilerParams(
            collective_id=0, has_side_effects=True, vmem_limit_bytes=62 * 1024 * 1024
        ),
    )(
        tok.T, w_gate, w_inner, w_state, w_step.T, k_inner, k_state,
        bias.reshape(1, -1), rate.reshape(1, -1), skip.reshape(1, -1), gain, w_out,
    )


def solution(mesh):
    return jax.shard_map(
        on_device,
        mesh=mesh,
        in_specs=(
            P("seq", "tp"), P(None, "tp"), P(None, "tp"), P(), P(None, "tp"), P(None, "tp"), P(),
            P("tp"), P("tp"), P("tp"), P("tp"), P("tp", None),
        ),
        out_specs=P(("seq", "tp"), None),
        check_vma=False,
    )
```
